256 devices in a mesh: band: 16 (over x_hi, z), grid: 16 (over y, x_lo, core).
Axes of the slice: x: 4 (x_hi: 2, x_lo: 2; x = x_hi * 2 + x_lo), y: 4, z: 8, core: 2. Of those that a mesh axis runs over, the one named last changes fastest.
Arguments:
- partial_density: float32 [16, 128, 128, 128], P('band', 'grid'), may hold values from 0.01 to 1
- node_index: int32 [128, 128, 128], P('grid'), may hold values from 0 to 19
- node_weight: float32 [4, 128, 128, 128], P(None, 'grid'), may hold values from 0 to 1
- node_slope: float32 [4, 128, 128, 128], P(None, 'grid'), may hold values from -6 to 6
- kernel_table: float32 [20, 20, 114], replicated, may hold values from -0.8 to 0.8, as said below
Outputs:
- potential: float32 [128, 128, 128], P('grid')
The draws below stay inside these ranges and needn't reach their ends.
Inputs may be any that keep to these rules, and one draw needn't show every extreme that they name: node_index(r) is the node at the lower end of the interval of q0 at r; nodes node_index - 1 to node_index + 2 carry the four weights. `kernel_table`: symmetric in its first two indices.
All inputs are finite; a program needn't handle non-finite values.
Results may differ from the reference program's by a relative error of at most 0.0003.
Values sent between devices are 32-bit elements; how exact they have to be, the bound alone decides.
No kernel may reach another device: no remote copies, remote signals or barrier semaphores. Data moves between devices by JAX's collectives and lax.ppermute only.
A program may use at most 64 MiB of HBM per device.

```python
import math
import jax
import jax.numpy as jnp
from jax import lax

N = 128
NA = 20
SHELLS = 114
GROUPS = 16


def draw_kernel_table(key, part):
    sample_values = jax.random.truncated_normal(key, -4.0, 4.0, (NA, NA, SHELLS), jnp.float32) * 0.2
    symmetric = 0.5 * (sample_values + jnp.transpose(sample_values, (1, 0, 2)))
    return symmetric


def touch_ends(array, own_key, least, largest):
    place = [jax.random.randint(jax.random.fold_in(own_key, axis), (), 0, length) for axis, length in enumerate(array.shape)]
    widest = array.shape.index(max(array.shape))
    next_to = place[:widest] + [(place[widest] + 1) % array.shape[widest]] + place[widest + 1:]
    return array.at[tuple(place)].set(least).at[tuple(next_to)].set(largest)


def block_scale(own_key, extent, split, smallest, high):
    level = 1.0
    for position, parts in split:
        steps = jax.random.uniform(jax.random.fold_in(jax.random.fold_in(own_key, 6), position), (parts,), jnp.float32, smallest / len(split), high / len(split))
        level = level * jnp.repeat(jnp.exp(steps), extent[position] // parts).reshape((-1,) + (1,) * (len(extent) - 1 - position))
    return level


def noise(key, shape, width, reach, pieces=(), kind=jnp.bfloat16):
    drawn = width * jax.random.normal(key, shape, jnp.float32)
    if pieces:
        drawn = drawn * block_scale(key, shape, pieces, -0.22, 0.18)
    return jnp.clip(drawn, -reach, reach).astype(kind)


def setup_inputs(seed: int = 0) -> dict:
    seeds = jax.random.split(jax.random.key(seed), 6)
    partial_density = jnp.clip(jnp.exp(math.log(1.0) - 4.6051702 * jax.random.uniform(seeds[0], (GROUPS, N, N, N), jnp.float32) ** block_scale(seeds[0], (GROUPS, N, N, N), ((0, 16), (1, 16)), -0.2, 0.2)), 0.01, 1.0)
    node_index = touch_ends(jax.random.randint(seeds[1], (N, N, N), 0, NA), jax.random.fold_in(seeds[1], 1), 0, NA - 1).astype(jnp.int32)
    node_weight = jnp.clip(1.0 * jax.random.uniform(seeds[2], (4, N, N, N), jnp.float32) ** block_scale(seeds[2], (4, N, N, N), ((1, 16),), -0.2, 0.2), 0.0, 1.0)
    node_slope = noise(seeds[3], (4, N, N, N), 1.0, 6.0, ((1, 16),), jnp.float32)
    kernel_table = draw_kernel_table(jax.random.fold_in(seeds[5], 71), 0)
    return {"partial_density": partial_density, "node_index": node_index, "node_weight": node_weight, "node_slope": node_slope, "kernel_table": kernel_table}


def frequency(length):
    positions = jnp.arange(length, dtype=jnp.int32)
    return jnp.where(positions < length // 2, positions, positions - length)

def shell_split(square_norm):
    root_value = jnp.sqrt(square_norm.astype(jnp.float32))
    shell_idx = root_value.astype(jnp.int32)
    shell_idx = shell_idx - (shell_idx * shell_idx > square_norm).astype(jnp.int32)
    shell_idx = shell_idx + ((shell_idx + 1) * (shell_idx + 1) <= square_norm).astype(jnp.int32)
    fraction = root_value - shell_idx.astype(jnp.float32)
    return (shell_idx, fraction)

def node_fields(count_nodes, intervals, weights):
    node_ids = jnp.arange(count_nodes, dtype=jnp.int32)
    summed = jnp.zeros((count_nodes,) + intervals.shape, jnp.float32)
    for offset in range(4):
        matched = node_ids[:, None, None, None] == (intervals + (offset - 1))[None]
        summed = summed + jnp.where(matched, weights[offset][None], jnp.zeros((), jnp.float32))
    return summed

def reference(partial_density, node_index, node_weight, node_slope, kernel_table):
    density = lax.optimization_barrier(jnp.sum(partial_density, axis=0))
    theta_fields = density[None] * node_fields(NA, node_index, node_weight)
    spectrum = jnp.fft.fftn(theta_fields, axes=(1, 2, 3))
    spec_real = jnp.real(spectrum)
    spec_imag = jnp.imag(spectrum)
    freq_all = frequency(N)
    plane_norm = freq_all[:, None] * freq_all[:, None] + freq_all[None, :] * freq_all[None, :]

    def mix_plane(plane_idx):
        freq_x = freq_all[plane_idx]
        shell_idx, fraction = shell_split(plane_norm + freq_x * freq_x)
        lower_values = kernel_table[:, :, shell_idx]
        upper_values = kernel_table[:, :, shell_idx + 1]
        kernel = (1.0 - fraction) * lower_values + fraction * upper_values
        plane_real = lax.dynamic_index_in_dim(spec_real, plane_idx, 1, keepdims=False)
        plane_imag = lax.dynamic_index_in_dim(spec_imag, plane_idx, 1, keepdims=False)
        out_real = jnp.einsum('abyz,ayz->byz', kernel, plane_real, precision=lax.Precision.HIGHEST)
        out_imag = jnp.einsum('abyz,ayz->byz', kernel, plane_imag, precision=lax.Precision.HIGHEST)
        return (out_real, out_imag)
    mixed_real, mixed_imag = lax.map(mix_plane, jnp.arange(N, dtype=jnp.int32))
    mixed = jnp.moveaxis(mixed_real + 1j * mixed_imag, 0, 1)
    fields = jnp.real(jnp.fft.ifftn(mixed, axes=(1, 2, 3)))
    return lax.optimization_barrier(jnp.sum(fields * node_fields(NA, node_index, node_slope), axis=0))
```

```python
import jax
import jax.numpy as jnp
import numpy as np
from jax import lax
from jax.experimental import pallas as pl
from jax.experimental.pallas import tpu as pltpu
from jax.sharding import PartitionSpec as P

N = 128
NA = 20
HALF_NA = 10
PAIRS = NA * (NA + 1) // 2
PAIR_ROWS = 216
POINTS = 64
ROWS = 5


def cas_table():
    idx = np.arange(N)
    angle = 2.0 * np.pi * ((idx[:, None] * idx[None, :]) % N) / N
    return np.cos(angle) + np.sin(angle)


def split_constant(table):
    high = jnp.asarray(table, jnp.float32).astype(jnp.bfloat16)
    low = (jnp.asarray(table, jnp.float32) - high.astype(jnp.float32)).astype(jnp.bfloat16)
    return jnp.stack([high, low])


def split_value(value):
    high = value.astype(jnp.bfloat16)
    low = (value - high.astype(jnp.float32)).astype(jnp.bfloat16)
    return high, low


def product(left, right, dims=((1,), (0,))):
    dot = lambda a, b: lax.dot_general(a, b, (dims, ((), ())), preferred_element_type=jnp.float32)
    return dot(left[0], right[0]) + (dot(left[0], right[1]) + dot(left[1], right[0]))


def node_sum(rel, fields, node):
    out = jnp.zeros_like(fields[0])
    for offset in range(4):
        out = jnp.where(rel == node - (offset - 1), fields[offset], out)
    return out


def frequency(positions):
    return jnp.where(positions < N // 2, positions, positions - N)


def phi_kernel(place_ref, table_ref, out_ref, flat_ref, shell_ref, fraction_ref, stage_ref):
    flat_ref[...] = jnp.zeros_like(flat_ref)
    start = 0
    for node in range(NA):
        count = NA - node
        flat_ref[start : start + count, 0 : table_ref.shape[2]] = table_ref[node, node:NA, :]
        start += count
    table = split_value(flat_ref[...])
    freq_y = frequency(place_ref[0])
    point = lax.broadcasted_iota(jnp.int32, (POINTS, N), 0)
    freq_z = frequency(point + place_ref[1] * POINTS)
    freq_x = frequency(lax.broadcasted_iota(jnp.int32, (POINTS, N), 1))
    square = freq_x * freq_x + freq_z * freq_z + freq_y * freq_y
    root = jnp.sqrt(square.astype(jnp.float32))
    shell = root.astype(jnp.int32)
    shell = shell - (shell * shell > square).astype(jnp.int32)
    shell = shell + ((shell + 1) * (shell + 1) <= square).astype(jnp.int32)
    shell_ref[...] = shell
    fraction_ref[...] = root - shell.astype(jnp.float32)
    row = lax.broadcasted_iota(jnp.int32, (N, N), 0)

    def weights(at):
        low = shell_ref[pl.ds(at, 1), :]
        part = fraction_ref[pl.ds(at, 1), :]
        return jnp.where(row == low, 1.0 - part, jnp.where(row == low + 1, part, 0.0))

    def group(step, carry):
        for pair in range(4):
            first = step * 8 + pair * 2
            both = jnp.concatenate([weights(first), weights(first + 1)], axis=1)
            value = product(table, split_value(both))
            stage_ref[pair * 2 * PAIR_ROWS : (pair * 2 + 1) * PAIR_ROWS, :] = value[:, :N]
            stage_ref[(pair * 2 + 1) * PAIR_ROWS : (pair * 2 + 2) * PAIR_ROWS, :] = value[:, N:]
        for item in range(PAIRS):
            out_ref[item, pl.ds(step * 8, 8), :] = stage_ref[pl.ds(item, 8, stride=PAIR_ROWS), :]
        return carry

    lax.fori_loop(0, POINTS // 8, group, 0)


def forward_kernel(place_ref, own_ref, other_ref, index_ref, weight_ref, cas_ref, out_ref):
    parity = place_ref[1]
    own, other = own_ref[...], other_ref[...]
    first = parity == 0
    density = jnp.concatenate([jnp.where(first, own, other), jnp.where(first, other, own)], axis=0)
    rel = index_ref[0] - parity * HALF_NA
    fields = [density * weight_ref[offset, 0] for offset in range(4)]
    cas = (cas_ref[0], cas_ref[1])
    lane = lax.broadcasted_iota(jnp.int32, (N, N), 1)
    for pair in range(ROWS):
        waves = []
        for node in (2 * pair, 2 * pair + 1):
            along_z = product(split_value(node_sum(rel, fields, node)), cas)
            waves.append(product(cas, split_value(along_z)))
        even, odd = waves
        out_ref[pl.ds(pair, N, stride=2 * ROWS), :] = jnp.where(
            lane < POINTS, even, pltpu.roll(odd, POINTS, 1)
        )
        out_ref[pl.ds(ROWS + pair, N, stride=2 * ROWS), :] = jnp.where(
            lane < POINTS, pltpu.roll(even, POINTS, 1), odd
        )


def mix_kernel(data_ref, cas_ref, phi_ref, out_ref, spec_ref, mixed_ref):
    cas = (cas_ref[0], cas_ref[1])

    def lines(half, pair, at):
        return pl.ds((at * 2 + half) * 16 * ROWS + pair, 16, stride=ROWS)

    for half in range(2):
        for pair in range(ROWS):
            block = jnp.concatenate([data_ref[lines(half, pair, at), :] for at in range(8)], axis=0)
            start = (half * ROWS + pair) * N
            spec_ref[start : start + N, :] = product(split_value(block.T), cas)

    def group(step, carry):
        spec = [spec_ref[pl.ds(node * POINTS + step * 8, 8), :] for node in range(NA)]
        total = [None] * NA
        item = 0
        for a in range(NA):
            for b in range(a, NA):
                phi = phi_ref[item, pl.ds(step * 8, 8), :]
                item += 1
                term = phi * spec[a]
                total[b] = term if total[b] is None else total[b] + term
                if a != b:
                    term = phi * spec[b]
                    total[a] = term if total[a] is None else total[a] + term
        for b in range(NA):
            mixed_ref[pl.ds(b * POINTS + step * 8, 8), :] = total[b]
        return carry

    lax.fori_loop(0, POINTS // 8, group, 0)
    for half in range(2):
        for pair in range(ROWS):
            start = (half * ROWS + pair) * N
            block = product(cas, split_value(mixed_ref[start : start + N, :]), ((1,), (1,)))
            for at in range(8):
                out_ref[lines(half, pair, at), :] = block[at * 16 : at * 16 + 16]


def inverse_kernel(place_ref, data_ref, index_ref, slope_ref, cas_ref, keep_ref, send_ref, sum_ref):
    parity = place_ref[1]
    rel = index_ref[0] - parity * HALF_NA
    slopes = [slope_ref[offset, 0] for offset in range(4)]
    cas = (cas_ref[0], cas_ref[1])
    lane = lax.broadcasted_iota(jnp.int32, (N, N), 1)
    total = jnp.zeros((N, N), jnp.float32)
    for pair in range(ROWS):
        lower = data_ref[pl.ds(pair, N, stride=2 * ROWS), :]
        upper = data_ref[pl.ds(ROWS + pair, N, stride=2 * ROWS), :]
        even = jnp.where(lane < POINTS, lower, pltpu.roll(upper, POINTS, 1))
        odd = jnp.where(lane < POINTS, pltpu.roll(lower, POINTS, 1), upper)
        for node, wave in ((2 * pair, even), (2 * pair + 1, odd)):
            along_y = product(cas, split_value(wave))
            field = product(split_value(along_y), cas)
            total = total + field * node_sum(rel, slopes, node)
    sum_ref[...] = total * (1.0 / float(N) ** 3)
    keep_ref[...] = sum_ref[pl.ds(parity * 64, 64), :]
    send_ref[...] = sum_ref[pl.ds(64 - parity * 64, 64), :]


def vmem():
    return pl.BlockSpec(memory_space=pltpu.VMEM)


def per_device(partial_density, node_index, node_weight, node_slope, kernel_table):
    band_at = lax.axis_index("band")
    grid_at = lax.axis_index("grid")
    table = cas_table()
    cas = split_constant(table)
    x_order = np.arange(N).reshape(16, 8).T.reshape(-1)
    cas_x = split_constant(table[x_order])
    plane = jnp.stack([band_at // 2, band_at % 2]).astype(jnp.int32)
    wave = jnp.stack([band_at * 8 + grid_at // 2, grid_at % 2]).astype(jnp.int32)
    partner = [(i, i ^ 1) for i in range(16)]
    axes = ("band", "grid")
    f32 = jnp.float32

    phi = pl.pallas_call(
        phi_kernel,
        out_shape=jax.ShapeDtypeStruct((PAIRS, POINTS, N), f32),
        in_specs=[pl.BlockSpec(memory_space=pltpu.SMEM), vmem()],
        out_specs=vmem(),
        scratch_shapes=[
            pltpu.VMEM((PAIR_ROWS, N), f32),
            pltpu.VMEM((POINTS, N), jnp.int32),
            pltpu.VMEM((POINTS, N), f32),
            pltpu.VMEM((8 * PAIR_ROWS, N), f32),
        ],
        compiler_params=pltpu.CompilerParams(vmem_limit_bytes=16 << 20),
        cost_estimate=pl.CostEstimate(flops=4 * 10**9, bytes_accessed=8 << 20, transcendentals=0),
        name="phi",
    )(wave, kernel_table)

    parts = lax.all_to_all(
        partial_density.reshape(16, 64, N), "band", 0, 0, tiled=True
    )
    own = jnp.sum(parts, axis=0)
    other = lax.ppermute(own, "band", partner)

    def plane_of(at, place):
        return (place[0], 0, 0)

    def planes_of(at, place):
        return (0, place[0], 0, 0)

    def whole(rank):
        return lambda at, place: (0,) * rank

    lines = pl.pallas_call(
        forward_kernel,
        out_shape=jax.ShapeDtypeStruct((256 * ROWS, N), f32),
        grid_spec=pltpu.PrefetchScalarGridSpec(
            num_scalar_prefetch=1,
            grid=(1,),
            in_specs=[
                pl.BlockSpec((64, N), whole(2)),
                pl.BlockSpec((64, N), whole(2)),
                pl.BlockSpec((1, N, N), plane_of),
                pl.BlockSpec((4, 1, N, N), planes_of),
                pl.BlockSpec((2, N, N), whole(3)),
            ],
            out_specs=pl.BlockSpec((256 * ROWS, N), whole(2)),
        ),
        compiler_params=pltpu.CompilerParams(vmem_limit_bytes=16 << 20),
        name="forward",
    )(plane, own, other, node_index, node_weight, cas)
    lines = lax.all_to_all(lines.reshape(256, 1, ROWS * N), axes, 0, 0, tiled=True)
    lines = lines.reshape(256 * ROWS, N)
    lines = pl.pallas_call(
        mix_kernel,
        out_shape=jax.ShapeDtypeStruct((256 * ROWS, N), f32),
        in_specs=[vmem(), vmem(), vmem()],
        out_specs=vmem(),
        scratch_shapes=[pltpu.VMEM((NA * POINTS, N), f32), pltpu.VMEM((NA * POINTS, N), f32)],
        compiler_params=pltpu.CompilerParams(vmem_limit_bytes=24 << 20),
        name="mix",
    )(lines, cas_x, phi)
    lines = lax.all_to_all(lines.reshape(256, 1, ROWS * N), axes, 0, 0, tiled=True)
    lines = lines.reshape(256 * ROWS, N)
    keep, send = pl.pallas_call(
        inverse_kernel,
        out_shape=[jax.ShapeDtypeStruct((64, N), f32), jax.ShapeDtypeStruct((64, N), f32)],
        grid_spec=pltpu.PrefetchScalarGridSpec(
            num_scalar_prefetch=1,
            grid=(1,),
            in_specs=[
                pl.BlockSpec((256 * ROWS, N), whole(2)),
                pl.BlockSpec((1, N, N), plane_of),
                pl.BlockSpec((4, 1, N, N), planes_of),
                pl.BlockSpec((2, N, N), whole(3)),
            ],
            out_specs=[pl.BlockSpec((64, N), whole(2)), pl.BlockSpec((64, N), whole(2))],
            scratch_shapes=[pltpu.VMEM((N, N), f32)],
        ),
        compiler_params=pltpu.CompilerParams(vmem_limit_bytes=16 << 20),
        name="inverse",
    )(plane, lines, node_index, node_slope, cas)
    share = keep + lax.ppermute(send, "band", partner)
    gathered = lax.all_to_all(
        jnp.broadcast_to(share[None], (16, 64, N)), "band", 0, 0, tiled=True
    )
    return gathered.reshape(8, N, N)


def solution(mesh):
    placed = (
        P("band", "grid", None, None),
        P("grid", None, None),
        P(None, "grid", None, None),
        P(None, "grid", None, None),
        P(),
    )
    return jax.shard_map(
        per_device, mesh=mesh, in_specs=placed, out_specs=P("grid", None, None), check_vma=False
    )
```

```python
import jax
import jax.numpy as jnp
import numpy as np
from jax import lax
from jax.experimental import pallas as pl
from jax.experimental.pallas import tpu as pltpu
from jax.sharding import PartitionSpec as P

N = 128
NA = 20
HALF_NA = 10
PAIRS = NA * (NA + 1) // 2
PAIR_ROWS = 216
POINTS = 64
ROWS = 5
GROUPS = POINTS // 8


def cas_table():
    idx = np.arange(N)
    angle = 2.0 * np.pi * ((idx[:, None] * idx[None, :]) % N) / N
    return np.cos(angle) + np.sin(angle)


def split_constant(table):
    high = jnp.asarray(table, jnp.float32).astype(jnp.bfloat16)
    low = (jnp.asarray(table, jnp.float32) - high.astype(jnp.float32)).astype(jnp.bfloat16)
    return jnp.stack([high, low])


def split_value(value):
    high = value.astype(jnp.bfloat16)
    low = (value - high.astype(jnp.float32)).astype(jnp.bfloat16)
    return high, low


def product(left, right, dims=((1,), (0,))):
    dot = lambda a, b: lax.dot_general(a, b, (dims, ((), ())), preferred_element_type=jnp.float32)
    return dot(left[0], right[0]) + (dot(left[0], right[1]) + dot(left[1], right[0]))


def node_sum(rel, fields, node):
    out = jnp.zeros_like(fields[0])
    for offset in range(4):
        out = jnp.where(rel == node - (offset - 1), fields[offset], out)
    return out


def frequency(positions):
    return jnp.where(positions < N // 2, positions, positions - N)


def phi_kernel(place_ref, table_ref, out_ref, flat_ref, shell_ref, fraction_ref, stage_ref, group_ref, sems):
    flat_ref[...] = jnp.zeros_like(flat_ref)
    start = 0
    for node in range(NA):
        count = NA - node
        flat_ref[start : start + count, 0 : table_ref.shape[2]] = table_ref[node, node:NA, :]
        start += count
    table = split_value(flat_ref[...])
    freq_y = frequency(place_ref[0])
    point = lax.broadcasted_iota(jnp.int32, (POINTS, N), 0)
    freq_z = frequency(point + place_ref[1] * POINTS)
    freq_x = frequency(lax.broadcasted_iota(jnp.int32, (POINTS, N), 1))
    square = freq_x * freq_x + freq_z * freq_z + freq_y * freq_y
    root = jnp.sqrt(square.astype(jnp.float32))
    shell = root.astype(jnp.int32)
    shell = shell - (shell * shell > square).astype(jnp.int32)
    shell = shell + ((shell + 1) * (shell + 1) <= square).astype(jnp.int32)
    shell_ref[...] = shell
    fraction_ref[...] = root - shell.astype(jnp.float32)
    row = lax.broadcasted_iota(jnp.int32, (N, N), 0)

    def weights(at):
        low = shell_ref[pl.ds(at, 1), :]
        part = fraction_ref[pl.ds(at, 1), :]
        return jnp.where(row == low, 1.0 - part, jnp.where(row == low + 1, part, 0.0))

    def put(step):
        slot = step % 2
        return pltpu.make_async_copy(group_ref.at[slot], out_ref.at[step], sems.at[slot])

    def group(step, carry):
        for pair in range(4):
            first = step * 8 + pair * 2
            both = jnp.concatenate([weights(first), weights(first + 1)], axis=1)
            value = product(table, split_value(both))
            stage_ref[pair * 2 * PAIR_ROWS : (pair * 2 + 1) * PAIR_ROWS, :] = value[:, :N]
            stage_ref[(pair * 2 + 1) * PAIR_ROWS : (pair * 2 + 2) * PAIR_ROWS, :] = value[:, N:]

        @pl.when(step >= 2)
        def _():
            put(step - 2).wait()

        for item in range(PAIRS):
            group_ref[step % 2, item] = stage_ref[pl.ds(item, 8, stride=PAIR_ROWS), :]
        put(step).start()
        return carry

    lax.fori_loop(0, GROUPS, group, 0)
    put(GROUPS - 2).wait()
    put(GROUPS - 1).wait()


def fields_kernel(
    place_ref, index_ref, weight_ref, slope_ref, theta_out, slope_out,
    index_buf, weight_buf, slope_buf, sems,
):
    plane = place_ref[0]
    copies = [
        pltpu.make_async_copy(index_ref.at[plane], index_buf, sems.at[0]),
        pltpu.make_async_copy(weight_ref.at[:, plane], weight_buf, sems.at[1]),
        pltpu.make_async_copy(slope_ref.at[:, plane], slope_buf, sems.at[2]),
    ]
    for copy in copies:
        copy.start()
    for copy in copies:
        copy.wait()
    rel = index_buf[...] - place_ref[1] * HALF_NA
    for buf, out_ref in ((weight_buf, theta_out), (slope_buf, slope_out)):
        fields = [buf[offset] for offset in range(4)]
        for node in range(HALF_NA):
            out_ref[node] = node_sum(rel, fields, node)


def load_kernel(own_ref, phi_far, theta_far, cas_far, phi_ref, theta_ref, cas_ref, phi_sems, sems):
    copies = [
        pltpu.make_async_copy(theta_far, theta_ref, sems.at[0]),
        pltpu.make_async_copy(cas_far, cas_ref, sems.at[1]),
    ]
    copies += [
        pltpu.make_async_copy(phi_far.at[step], phi_ref.at[step], phi_sems.at[step])
        for step in range(GROUPS)
    ]
    for copy in copies:
        copy.start()
    for copy in copies:
        copy.wait()


def forward_kernel(place_ref, own_ref, other_ref, coefficient_ref, cas_ref, out_ref):
    own, other = own_ref[...], other_ref[...]
    first = place_ref[1] == 0
    density = jnp.concatenate([jnp.where(first, own, other), jnp.where(first, other, own)], axis=0)
    cas = (cas_ref[0], cas_ref[1])
    lane = lax.broadcasted_iota(jnp.int32, (N, N), 1)
    for pair in range(ROWS):
        waves = []
        for node in (2 * pair, 2 * pair + 1):
            along_z = product(split_value(density * coefficient_ref[node]), cas)
            waves.append(product(cas, split_value(along_z)))
        even, odd = waves
        out_ref[pl.ds(pair, N, stride=2 * ROWS), :] = jnp.where(
            lane < POINTS, even, pltpu.roll(odd, POINTS, 1)
        )
        out_ref[pl.ds(ROWS + pair, N, stride=2 * ROWS), :] = jnp.where(
            lane < POINTS, pltpu.roll(even, POINTS, 1), odd
        )


def mix_kernel(data_ref, cas_ref, phi_ref, out_ref, spec_ref, mixed_ref):
    cas = (cas_ref[0], cas_ref[1])

    def lines(half, pair, at):
        return pl.ds((at * 2 + half) * 16 * ROWS + pair, 16, stride=ROWS)

    for half in range(2):
        for pair in range(ROWS):
            block = jnp.concatenate([data_ref[lines(half, pair, at), :] for at in range(8)], axis=0)
            start = (half * ROWS + pair) * N
            spec_ref[start : start + N, :] = product(split_value(block.T), cas)

    def group(step, carry):
        spec = [spec_ref[pl.ds(node * POINTS + step * 8, 8), :] for node in range(NA)]
        total = [None] * NA
        item = 0
        for a in range(NA):
            for b in range(a, NA):
                phi = phi_ref[step, item]
                item += 1
                term = phi * spec[a]
                total[b] = term if total[b] is None else total[b] + term
                if a != b:
                    term = phi * spec[b]
                    total[a] = term if total[a] is None else total[a] + term
        for b in range(NA):
            mixed_ref[pl.ds(b * POINTS + step * 8, 8), :] = total[b]
        return carry

    lax.fori_loop(0, GROUPS, group, 0)
    for half in range(2):
        for pair in range(ROWS):
            start = (half * ROWS + pair) * N
            block = product(cas, split_value(mixed_ref[start : start + N, :]), ((1,), (1,)))
            for at in range(8):
                out_ref[lines(half, pair, at), :] = block[at * 16 : at * 16 + 16]


def inverse_kernel(place_ref, data_ref, coefficient_ref, cas_ref, keep_ref, send_ref, sum_ref):
    parity = place_ref[1]
    cas = (cas_ref[0], cas_ref[1])
    lane = lax.broadcasted_iota(jnp.int32, (N, N), 1)
    total = jnp.zeros((N, N), jnp.float32)
    for pair in range(ROWS):
        lower = data_ref[pl.ds(pair, N, stride=2 * ROWS), :]
        upper = data_ref[pl.ds(ROWS + pair, N, stride=2 * ROWS), :]
        even = jnp.where(lane < POINTS, lower, pltpu.roll(upper, POINTS, 1))
        odd = jnp.where(lane < POINTS, pltpu.roll(lower, POINTS, 1), upper)
        for node, wave in ((2 * pair, even), (2 * pair + 1, odd)):
            along_y = product(cas, split_value(wave))
            field = product(split_value(along_y), cas)
            total = total + field * coefficient_ref[node]
    sum_ref[...] = total * (1.0 / float(N) ** 3)
    keep_ref[...] = sum_ref[pl.ds(parity * 64, 64), :]
    send_ref[...] = sum_ref[pl.ds(64 - parity * 64, 64), :]


def vmem():
    return pl.BlockSpec(memory_space=pltpu.VMEM)


def scalars():
    return pl.BlockSpec(memory_space=pltpu.SMEM)


def anywhere():
    return pl.BlockSpec(memory_space=pl.ANY)


def far(value):
    return pltpu.with_memory_space_constraint(value, pltpu.HBM)


def per_device(partial_density, node_index, node_weight, node_slope, kernel_table):
    band_at = lax.axis_index("band")
    grid_at = lax.axis_index("grid")
    table = cas_table()
    cas = split_constant(table)
    x_order = np.arange(N).reshape(16, 8).T.reshape(-1)
    cas_x = split_constant(table[x_order])
    plane = jnp.stack([band_at // 2, band_at % 2]).astype(jnp.int32)
    wave = jnp.stack([band_at * 8 + grid_at // 2, grid_at % 2]).astype(jnp.int32)
    partner = [(i, i ^ 1) for i in range(16)]
    axes = ("band", "grid")
    f32 = jnp.float32

    phi_far = pl.pallas_call(
        phi_kernel,
        out_shape=pltpu.HBM((GROUPS, PAIRS, 8, N), f32),
        in_specs=[scalars(), vmem()],
        out_specs=anywhere(),
        scratch_shapes=[
            pltpu.VMEM((PAIR_ROWS, N), f32),
            pltpu.VMEM((POINTS, N), jnp.int32),
            pltpu.VMEM((POINTS, N), f32),
            pltpu.VMEM((8 * PAIR_ROWS, N), f32),
            pltpu.VMEM((2, PAIRS, 8, N), f32),
            pltpu.SemaphoreType.DMA((2,)),
        ],
        compiler_params=pltpu.CompilerParams(vmem_limit_bytes=8 << 20),
        cost_estimate=pl.CostEstimate(flops=4 * 10**9, bytes_accessed=8 << 20, transcendentals=0),
        name="phi",
    )(wave, kernel_table)

    theta, slope = pl.pallas_call(
        fields_kernel,
        out_shape=[pltpu.HBM((HALF_NA, N, N), f32)] * 2,
        in_specs=[scalars()] + [anywhere()] * 3,
        out_specs=[vmem()] * 2,
        scratch_shapes=[
            pltpu.VMEM((N, N), jnp.int32),
            pltpu.VMEM((4, N, N), f32),
            pltpu.VMEM((4, N, N), f32),
            pltpu.SemaphoreType.DMA((3,)),
        ],
        compiler_params=pltpu.CompilerParams(vmem_limit_bytes=4 << 20),
        cost_estimate=pl.CostEstimate(flops=10**8, bytes_accessed=2 << 20, transcendentals=0),
        name="fields",
    )(plane, far(node_index), far(node_weight), far(node_slope))
    parts = lax.all_to_all(partial_density.reshape(16, 64, N), "band", 0, 0, tiled=True)
    own = jnp.sum(parts, axis=0)
    own, phi_far, slope, theta_far = lax.optimization_barrier((own, phi_far, slope, theta))
    other = lax.ppermute(own, "band", partner)
    phi, theta, cas_near = pl.pallas_call(
        load_kernel,
        out_shape=[
            pltpu.VMEM(phi_far.shape, f32),
            pltpu.VMEM(theta_far.shape, f32),
            pltpu.VMEM(cas.shape, cas.dtype),
        ],
        in_specs=[anywhere()] * 4,
        out_specs=[vmem()] * 3,
        scratch_shapes=[pltpu.SemaphoreType.DMA((GROUPS,)), pltpu.SemaphoreType.DMA((2,))],
        compiler_params=pltpu.CompilerParams(vmem_limit_bytes=2 << 20),
        cost_estimate=pl.CostEstimate(flops=10**9, bytes_accessed=8 << 20, transcendentals=0),
        name="load",
    )(own, far(phi_far), far(theta_far), far(cas))
    lines = pl.pallas_call(
        forward_kernel,
        out_shape=jax.ShapeDtypeStruct((256 * ROWS, N), f32),
        in_specs=[pl.BlockSpec(memory_space=pltpu.SMEM)] + [vmem()] * 4,
        out_specs=vmem(),
        compiler_params=pltpu.CompilerParams(vmem_limit_bytes=12 << 20),
        name="forward",
    )(plane, own, other, theta, cas_near)
    lines = lax.all_to_all(lines.reshape(256, 1, ROWS * N), axes, 0, 0, tiled=True)
    lines = lines.reshape(256 * ROWS, N)
    lines = pl.pallas_call(
        mix_kernel,
        out_shape=jax.ShapeDtypeStruct((256 * ROWS, N), f32),
        in_specs=[vmem(), vmem(), vmem()],
        out_specs=vmem(),
        scratch_shapes=[pltpu.VMEM((NA * POINTS, N), f32), pltpu.VMEM((NA * POINTS, N), f32)],
        compiler_params=pltpu.CompilerParams(vmem_limit_bytes=24 << 20),
        name="mix",
    )(lines, cas_x, phi)
    lines = lax.all_to_all(lines.reshape(256, 1, ROWS * N), axes, 0, 0, tiled=True)
    lines = lines.reshape(256 * ROWS, N)
    keep, send = pl.pallas_call(
        inverse_kernel,
        out_shape=[jax.ShapeDtypeStruct((64, N), f32), jax.ShapeDtypeStruct((64, N), f32)],
        in_specs=[pl.BlockSpec(memory_space=pltpu.SMEM)] + [vmem()] * 3,
        out_specs=[vmem(), vmem()],
        scratch_shapes=[pltpu.VMEM((N, N), f32)],
        compiler_params=pltpu.CompilerParams(vmem_limit_bytes=12 << 20),
        name="inverse",
    )(plane, lines, slope, cas)
    share = keep + lax.ppermute(send, "band", partner)
    gathered = lax.all_to_all(
        jnp.broadcast_to(share[None], (16, 64, N)), "band", 0, 0, tiled=True
    )
    return gathered.reshape(8, N, N)


def solution(mesh):
    placed = (
        P("band", "grid", None, None),
        P("grid", None, None),
        P(None, "grid", None, None),
        P(None, "grid", None, None),
        P(),
    )
    return jax.shard_map(
        per_device, mesh=mesh, in_specs=placed, out_specs=P("grid", None, None), check_vma=False
    )
```

```python
import jax
import jax.numpy as jnp
import numpy as np
from jax import lax
from jax.experimental import pallas as pl
from jax.experimental.pallas import tpu as pltpu
from jax.sharding import PartitionSpec as P

N = 128
NA = 20
HALF_NA = 10
PAIRS = NA * (NA + 1) // 2
PAIR_ROWS = 216
POINTS = 64
ROWS = 5
GROUPS = POINTS // 8
NEAR = 7


def cas_table():
    idx = np.arange(N)
    angle = 2.0 * np.pi * ((idx[:, None] * idx[None, :]) % N) / N
    return np.cos(angle) + np.sin(angle)


def split_constant(table):
    high = jnp.asarray(table, jnp.float32).astype(jnp.bfloat16)
    low = (jnp.asarray(table, jnp.float32) - high.astype(jnp.float32)).astype(jnp.bfloat16)
    row = jnp.concatenate([high, low], axis=1)
    return jnp.concatenate([row, row], axis=0)


def split_value(value):
    high = value.astype(jnp.bfloat16)
    low = (value - high.astype(jnp.float32)).astype(jnp.bfloat16)
    return high, low


def product(left, right, dims=((1,), (0,))):
    dot = lambda a, b: lax.dot_general(a, b, (dims, ((), ())), preferred_element_type=jnp.float32)
    return dot(left[0], right[0]) + (dot(left[0], right[1]) + dot(left[1], right[0]))


def halves_added(value):
    return value[:, :N] + value[:, N:]


def rows_times(value, wide):
    parts = jnp.concatenate(split_value(value), axis=1)
    return halves_added(jnp.dot(parts, wide, preferred_element_type=jnp.float32))


def times_block(wide, value):
    parts = jnp.concatenate(split_value(value), axis=1)
    parts = jnp.concatenate([parts, parts], axis=0)
    return halves_added(jnp.dot(wide[:N], parts, preferred_element_type=jnp.float32))


def times_block_turned(wide, value):
    parts = jnp.concatenate(split_value(value), axis=0)
    parts = jnp.concatenate([parts, parts], axis=1)
    dims = (((1,), (1,)), ((), ()))
    return halves_added(
        lax.dot_general(wide[:N], parts, dims, preferred_element_type=jnp.float32)
    )


def node_sum(rel, fields, node):
    out = jnp.zeros_like(fields[0])
    for offset in range(4):
        out = jnp.where(rel == node - (offset - 1), fields[offset], out)
    return out


def frequency(positions):
    return jnp.where(positions < N // 2, positions, positions - N)


def phi_kernel(table_ref, out_ref, flat_ref, shell_ref, fraction_ref, stage_ref, group_ref, sems):
    flat_ref[...] = jnp.zeros_like(flat_ref)
    start = 0
    for node in range(NA):
        count = NA - node
        flat_ref[start : start + count, 0 : table_ref.shape[2]] = table_ref[node, node:NA, :]
        start += count
    table = split_value(flat_ref[...])
    band_at, grid_at = lax.axis_index("band"), lax.axis_index("grid")
    freq_y = frequency(band_at * 8 + grid_at // 2)
    point = lax.broadcasted_iota(jnp.int32, (POINTS, N), 0)
    freq_z = frequency(point + grid_at % 2 * POINTS)
    freq_x = frequency(lax.broadcasted_iota(jnp.int32, (POINTS, N), 1))
    square = freq_x * freq_x + freq_z * freq_z + freq_y * freq_y
    root = jnp.sqrt(square.astype(jnp.float32))
    shell = root.astype(jnp.int32)
    shell = shell - (shell * shell > square).astype(jnp.int32)
    shell = shell + ((shell + 1) * (shell + 1) <= square).astype(jnp.int32)
    shell_ref[...] = shell
    fraction_ref[...] = root - shell.astype(jnp.float32)
    row = lax.broadcasted_iota(jnp.int32, (N, N), 0)

    def weights(at):
        low = shell_ref[pl.ds(at, 1), :]
        part = fraction_ref[pl.ds(at, 1), :]
        return jnp.where(row == low, 1.0 - part, jnp.where(row == low + 1, part, 0.0))

    def put(step):
        slot = step % 2
        return pltpu.make_async_copy(group_ref.at[slot], out_ref.at[step], sems.at[slot])

    def group(step, carry):
        for pair in range(4):
            first = step * 8 + pair * 2
            both = jnp.concatenate([weights(first), weights(first + 1)], axis=1)
            value = product(table, split_value(both))
            stage_ref[pair * 2 * PAIR_ROWS : (pair * 2 + 1) * PAIR_ROWS, :] = value[:, :N]
            stage_ref[(pair * 2 + 1) * PAIR_ROWS : (pair * 2 + 2) * PAIR_ROWS, :] = value[:, N:]

        @pl.when(step >= 2)
        def _():
            put(step - 2).wait()

        for item in range(PAIRS):
            group_ref[step % 2, item] = stage_ref[pl.ds(item, 8, stride=PAIR_ROWS), :]
        put(step).start()
        return carry

    lax.fori_loop(0, GROUPS, group, 0)
    put(GROUPS - 2).wait()
    put(GROUPS - 1).wait()


def fields_kernel(
    index_ref, weight_ref, slope_ref, theta_out, slope_out,
    index_buf, weight_buf, slope_buf, sems,
):
    band_at = lax.axis_index("band")
    plane = band_at // 2
    copies = [
        pltpu.make_async_copy(index_ref.at[plane], index_buf, sems.at[0]),
        pltpu.make_async_copy(weight_ref.at[:, plane], weight_buf, sems.at[1]),
        pltpu.make_async_copy(slope_ref.at[:, plane], slope_buf, sems.at[2]),
    ]
    for copy in copies:
        copy.start()
    for copy in copies:
        copy.wait()
    rel = index_buf[...] - band_at % 2 * HALF_NA
    for buf, out_ref in ((weight_buf, theta_out), (slope_buf, slope_out)):
        fields = [buf[offset] for offset in range(4)]
        for node in range(HALF_NA):
            out_ref[node] = node_sum(rel, fields, node)


def load_kernel(own_ref, phi_far, theta_far, cas_far, phi_ref, theta_ref, cas_ref, phi_sems, sems):
    copies = [
        pltpu.make_async_copy(theta_far, theta_ref, sems.at[0]),
        pltpu.make_async_copy(cas_far, cas_ref, sems.at[1]),
    ]
    copies += [
        pltpu.make_async_copy(phi_far.at[step], phi_ref.at[step], phi_sems.at[step])
        for step in range(NEAR)
    ]
    for copy in copies:
        copy.start()
    for copy in copies:
        copy.wait()


def forward_kernel(own_ref, other_ref, coefficient_ref, cas_ref, out_ref):
    own, other = own_ref[...], other_ref[...]
    first = lax.axis_index("band") % 2 == 0
    density = jnp.concatenate([jnp.where(first, own, other), jnp.where(first, other, own)], axis=0)
    cas = cas_ref[...]
    lane = lax.broadcasted_iota(jnp.int32, (N, N), 1)
    theta = density[None] * coefficient_ref[...]
    along_z = rows_times(theta.reshape(HALF_NA * N, N), cas)
    for pair in range(ROWS):
        waves = []
        for node in (2 * pair, 2 * pair + 1):
            waves.append(times_block(cas, along_z[node * N : (node + 1) * N]))
        even, odd = waves
        out_ref[pl.ds(pair, N, stride=2 * ROWS), :] = jnp.where(
            lane < POINTS, even, pltpu.roll(odd, POINTS, 1)
        )
        out_ref[pl.ds(ROWS + pair, N, stride=2 * ROWS), :] = jnp.where(
            lane < POINTS, pltpu.roll(even, POINTS, 1), odd
        )


def mix_kernel(data_ref, cas_ref, phi_ref, far_ref, out_ref, spec_ref, mixed_ref, late_ref, sems):
    cas = cas_ref[...]
    late = [
        pltpu.make_async_copy(far_ref.at[NEAR + step], late_ref.at[step], sems.at[step])
        for step in range(GROUPS - NEAR)
    ]
    for copy in late:
        copy.start()

    def lines(half, pair, at):
        return pl.ds((at * 2 + half) * 16 * ROWS + pair, 16, stride=ROWS)

    for half in range(2):
        for pair in range(ROWS):
            block = jnp.concatenate([data_ref[lines(half, pair, at), :] for at in range(8)], axis=0)
            start = (half * ROWS + pair) * N
            spec_ref[start : start + N, :] = rows_times(block.T, cas)

    def group(step, phi_at):
        spec = [spec_ref[pl.ds(node * POINTS + step * 8, 8), :] for node in range(NA)]
        total = [None] * NA
        item = 0
        for a in range(NA):
            for b in range(a, NA):
                phi = phi_at[item]
                item += 1
                term = phi * spec[a]
                total[b] = term if total[b] is None else total[b] + term
                if a != b:
                    term = phi * spec[b]
                    total[a] = term if total[a] is None else total[a] + term
        for b in range(NA):
            mixed_ref[pl.ds(b * POINTS + step * 8, 8), :] = total[b]

    def near(step, carry):
        group(step, phi_ref.at[step])
        return carry

    def far(step, carry):
        group(NEAR + step, late_ref.at[step])
        return carry

    lax.fori_loop(0, NEAR, near, 0)
    for copy in late:
        copy.wait()
    lax.fori_loop(0, GROUPS - NEAR, far, 0)
    for half in range(2):
        for pair in range(ROWS):
            start = (half * ROWS + pair) * N
            block = times_block_turned(cas, mixed_ref[start : start + N, :])
            for at in range(8):
                out_ref[lines(half, pair, at), :] = block[at * 16 : at * 16 + 16]


def inverse_kernel(data_ref, coefficient_ref, cas_ref, keep_ref, send_ref, sum_ref):
    parity = lax.axis_index("band") % 2
    cas = cas_ref[...]
    lane = lax.broadcasted_iota(jnp.int32, (N, N), 1)
    along_y = []
    for pair in range(ROWS):
        lower = data_ref[pl.ds(pair, N, stride=2 * ROWS), :]
        upper = data_ref[pl.ds(ROWS + pair, N, stride=2 * ROWS), :]
        along_y.append(
            times_block(cas, jnp.where(lane < POINTS, lower, pltpu.roll(upper, POINTS, 1)))
        )
        along_y.append(
            times_block(cas, jnp.where(lane < POINTS, pltpu.roll(lower, POINTS, 1), upper))
        )
    fields = rows_times(jnp.concatenate(along_y, axis=0), cas)
    total = fields[:N] * coefficient_ref[0]
    for node in range(1, HALF_NA):
        total = total + fields[node * N : (node + 1) * N] * coefficient_ref[node]
    sum_ref[...] = total * (1.0 / float(N) ** 3)
    keep_ref[...] = sum_ref[pl.ds(parity * 64, 64), :]
    send_ref[...] = sum_ref[pl.ds(64 - parity * 64, 64), :]


def vmem():
    return pl.BlockSpec(memory_space=pltpu.VMEM)


def anywhere():
    return pl.BlockSpec(memory_space=pl.ANY)


def far(value):
    return pltpu.with_memory_space_constraint(value, pltpu.HBM)


def per_device(partial_density, node_index, node_weight, node_slope, kernel_table):
    table = cas_table()
    cas = split_constant(table)
    x_order = np.arange(N).reshape(16, 8).T.reshape(-1)
    cas_x = split_constant(table[x_order])
    partner = [(i, i ^ 1) for i in range(16)]
    axes = ("band", "grid")
    f32 = jnp.float32

    phi_far = pl.pallas_call(
        phi_kernel,
        out_shape=pltpu.HBM((GROUPS, PAIRS, 8, N), f32),
        in_specs=[vmem()],
        out_specs=anywhere(),
        scratch_shapes=[
            pltpu.VMEM((PAIR_ROWS, N), f32),
            pltpu.VMEM((POINTS, N), jnp.int32),
            pltpu.VMEM((POINTS, N), f32),
            pltpu.VMEM((8 * PAIR_ROWS, N), f32),
            pltpu.VMEM((2, PAIRS, 8, N), f32),
            pltpu.SemaphoreType.DMA((2,)),
        ],
        compiler_params=pltpu.CompilerParams(vmem_limit_bytes=8 << 20),
        cost_estimate=pl.CostEstimate(flops=4 * 10**9, bytes_accessed=8 << 20, transcendentals=0),
        name="phi",
    )(kernel_table)

    theta, slope = pl.pallas_call(
        fields_kernel,
        out_shape=[pltpu.HBM((HALF_NA, N, N), f32)] * 2,
        in_specs=[anywhere()] * 3,
        out_specs=[vmem()] * 2,
        scratch_shapes=[
            pltpu.VMEM((N, N), jnp.int32),
            pltpu.VMEM((4, N, N), f32),
            pltpu.VMEM((4, N, N), f32),
            pltpu.SemaphoreType.DMA((3,)),
        ],
        compiler_params=pltpu.CompilerParams(vmem_limit_bytes=4 << 20),
        cost_estimate=pl.CostEstimate(flops=10**8, bytes_accessed=2 << 20, transcendentals=0),
        name="fields",
    )(far(node_index), far(node_weight), far(node_slope))
    parts = lax.all_to_all(partial_density.reshape(16, 64, N), "band", 0, 0, tiled=True)
    own = jnp.sum(parts, axis=0)
    own, phi_far, slope, theta_far = lax.optimization_barrier((own, phi_far, slope, theta))
    other = lax.ppermute(own, "band", partner)
    phi, theta, cas_near = pl.pallas_call(
        load_kernel,
        out_shape=[
            pltpu.VMEM((NEAR, PAIRS, 8, N), f32),
            pltpu.VMEM(theta_far.shape, f32),
            pltpu.VMEM(cas.shape, cas.dtype),
        ],
        in_specs=[anywhere()] * 4,
        out_specs=[vmem()] * 3,
        scratch_shapes=[pltpu.SemaphoreType.DMA((NEAR,)), pltpu.SemaphoreType.DMA((2,))],
        compiler_params=pltpu.CompilerParams(vmem_limit_bytes=2 << 20),
        cost_estimate=pl.CostEstimate(flops=10**9, bytes_accessed=8 << 20, transcendentals=0),
        name="load",
    )(own, far(phi_far), far(theta_far), far(cas))
    lines = pl.pallas_call(
        forward_kernel,
        out_shape=jax.ShapeDtypeStruct((256 * ROWS, N), f32),
        in_specs=[vmem()] * 4,
        out_specs=vmem(),
        compiler_params=pltpu.CompilerParams(vmem_limit_bytes=12 << 20),
        name="forward",
    )(own, other, theta, cas_near)
    lines = lax.all_to_all(lines.reshape(256, 1, ROWS * N), axes, 0, 0, tiled=True)
    lines = lines.reshape(256 * ROWS, N)
    lines = pl.pallas_call(
        mix_kernel,
        out_shape=jax.ShapeDtypeStruct((256 * ROWS, N), f32),
        in_specs=[vmem(), vmem(), vmem(), anywhere()],
        out_specs=vmem(),
        scratch_shapes=[
            pltpu.VMEM((NA * POINTS, N), f32),
            pltpu.VMEM((NA * POINTS, N), f32),
            pltpu.VMEM((GROUPS - NEAR, PAIRS, 8, N), f32),
            pltpu.SemaphoreType.DMA((GROUPS - NEAR,)),
        ],
        compiler_params=pltpu.CompilerParams(vmem_limit_bytes=24 << 20),
        name="mix",
    )(lines, cas_x, phi, far(phi_far))
    lines = lax.all_to_all(lines.reshape(256, 1, ROWS * N), axes, 0, 0, tiled=True)
    lines = lines.reshape(256 * ROWS, N)
    keep, send = pl.pallas_call(
        inverse_kernel,
        out_shape=[jax.ShapeDtypeStruct((64, N), f32), jax.ShapeDtypeStruct((64, N), f32)],
        in_specs=[vmem()] * 3,
        out_specs=[vmem(), vmem()],
        scratch_shapes=[pltpu.VMEM((N, N), f32)],
        compiler_params=pltpu.CompilerParams(vmem_limit_bytes=12 << 20),
        name="inverse",
    )(lines, slope, cas)
    share = keep + lax.ppermute(send, "band", partner)
    gathered = lax.all_to_all(
        jnp.broadcast_to(share[None], (16, 64, N)), "band", 0, 0, tiled=True
    )
    return gathered.reshape(8, N, N)


def solution(mesh):
    placed = (
        P("band", "grid", None, None),
        P("grid", None, None),
        P(None, "grid", None, None),
        P(None, "grid", None, None),
        P(),
    )
    return jax.shard_map(
        per_device, mesh=mesh, in_specs=placed, out_specs=P("grid", None, None), check_vma=False
    )
```

```python
import jax
import jax.numpy as jnp
import numpy as np
from jax import lax
from jax.experimental import pallas as pl
from jax.experimental.pallas import tpu as pltpu
from jax.sharding import PartitionSpec as P

N = 128
NA = 20
HALF_NA = 10
PAIRS = NA * (NA + 1) // 2
PAIR_ROWS = 216
POINTS = 64
ROWS = 5
GROUPS = POINTS // 8
NEAR = 7


def cas_table():
    idx = np.arange(N)
    angle = 2.0 * np.pi * ((idx[:, None] * idx[None, :]) % N) / N
    return np.cos(angle) + np.sin(angle)


def wave_order():
    sets = np.arange(32)
    other = np.where(sets == 0, 32, 64 - sets)
    return np.concatenate([sets, sets + 64, other, other + 64])


def half_table():
    idx = np.arange(64)
    order = wave_order().reshape(4, 32)[[0, 2]].reshape(-1)
    angle = 2.0 * np.pi * ((idx[:, None] * order[None, :]) % 64) / 64
    return np.cos(angle) + np.sin(angle)


def twist_table():
    angle = np.pi * np.arange(32) / 64
    factors = np.stack([np.cos(angle), np.sin(angle), np.sin(angle), -np.cos(angle)], axis=1)
    factors[0] = (1.0, 0.0, 0.0, 1.0)
    return jnp.asarray(np.repeat(factors.reshape(-1, 1), N, axis=1), jnp.float32)


def split_row(table):
    high = jnp.asarray(table, jnp.float32).astype(jnp.bfloat16)
    low = (jnp.asarray(table, jnp.float32) - high.astype(jnp.float32)).astype(jnp.bfloat16)
    return jnp.concatenate([high, low], axis=1)


def split_constant(table):
    row = split_row(table)
    return jnp.concatenate([row, row], axis=0)


def split_value(value):
    high = value.astype(jnp.bfloat16)
    low = (value - high.astype(jnp.float32)).astype(jnp.bfloat16)
    return high, low


def product(left, right, dims=((1,), (0,))):
    dot = lambda a, b: lax.dot_general(a, b, (dims, ((), ())), preferred_element_type=jnp.float32)
    return dot(left[0], right[0]) + (dot(left[0], right[1]) + dot(left[1], right[0]))


def halves_added(value):
    return value[:, :N] + value[:, N:]


def rows_times(value, wide):
    parts = jnp.concatenate(split_value(value), axis=1)
    return halves_added(jnp.dot(parts, wide, preferred_element_type=jnp.float32))


def times_block(row, value):
    parts = jnp.concatenate(split_value(value), axis=1)
    parts = jnp.concatenate([parts, parts], axis=0)
    return halves_added(jnp.dot(row, parts, preferred_element_type=jnp.float32))


def times_block_turned(wide, value):
    parts = jnp.concatenate(split_value(value), axis=0)
    parts = jnp.concatenate([parts, parts], axis=1)
    dims = (((1,), (1,)), ((), ()))
    return halves_added(
        lax.dot_general(wide[:N], parts, dims, preferred_element_type=jnp.float32)
    )


def turned_groups(items):
    items = list(items)
    group = lax.broadcasted_iota(jnp.int32, items[0].shape, 1) // 16
    for bit in (1, 2, 4):
        upper = group // bit % 2 == 1
        for at in range(8):
            if at & bit == 0:
                first, second = items[at], items[at | bit]
                items[at] = jnp.where(upper, pltpu.roll(second, bit * 16, 1), first)
                items[at | bit] = jnp.where(upper, second, pltpu.roll(first, N - bit * 16, 1))
    return items


def node_sum(rel, fields, node):
    out = jnp.zeros_like(fields[0])
    for offset in range(4):
        out = jnp.where(rel == node - (offset - 1), fields[offset], out)
    return out


def frequency(positions):
    return jnp.where(positions < N // 2, positions, positions - N)


def phi_kernel(table_ref, out_ref, flat_ref, shell_ref, fraction_ref, stage_ref, group_ref, sems):
    flat_ref[...] = jnp.zeros_like(flat_ref)
    start = 0
    for node in range(NA):
        count = NA - node
        flat_ref[start : start + count, 0 : table_ref.shape[2]] = table_ref[node, node:NA, :]
        start += count
    table = split_value(flat_ref[...])
    band_at, grid_at = lax.axis_index("band"), lax.axis_index("grid")
    wave_set = band_at * 2 + grid_at // 8
    point = lax.broadcasted_iota(jnp.int32, (POINTS, N), 0)
    slot = point // 16
    other = jnp.where(wave_set == 0, 32, 64 - wave_set)
    freq_y = frequency(jnp.where(slot < 2, wave_set, other) + slot % 2 * 64)
    freq_z = frequency(point % 16 + grid_at % 8 * 16)
    freq_x = frequency(lax.broadcasted_iota(jnp.int32, (POINTS, N), 1))
    square = freq_x * freq_x + freq_z * freq_z + freq_y * freq_y
    root = jnp.sqrt(square.astype(jnp.float32))
    shell = root.astype(jnp.int32)
    shell = shell - (shell * shell > square).astype(jnp.int32)
    shell = shell + ((shell + 1) * (shell + 1) <= square).astype(jnp.int32)
    shell_ref[...] = shell
    fraction_ref[...] = root - shell.astype(jnp.float32)
    row = lax.broadcasted_iota(jnp.int32, (N, N), 0)

    def weights(at):
        low = shell_ref[pl.ds(at, 1), :]
        part = fraction_ref[pl.ds(at, 1), :]
        return jnp.where(row == low, 1.0 - part, jnp.where(row == low + 1, part, 0.0))

    def put(step):
        slot = step % 2
        return pltpu.make_async_copy(group_ref.at[slot], out_ref.at[step], sems.at[slot])

    def group(step, carry):
        for pair in range(4):
            first = step * 8 + pair * 2
            both = jnp.concatenate([weights(first), weights(first + 1)], axis=1)
            value = product(table, split_value(both))
            stage_ref[pair * 2 * PAIR_ROWS : (pair * 2 + 1) * PAIR_ROWS, :] = value[:, :N]
            stage_ref[(pair * 2 + 1) * PAIR_ROWS : (pair * 2 + 2) * PAIR_ROWS, :] = value[:, N:]

        @pl.when(step >= 2)
        def _():
            put(step - 2).wait()

        for item in range(PAIRS):
            group_ref[step % 2, item] = stage_ref[pl.ds(item, 8, stride=PAIR_ROWS), :]
        put(step).start()
        return carry

    lax.fori_loop(0, GROUPS, group, 0)
    put(GROUPS - 2).wait()
    put(GROUPS - 1).wait()


def fields_kernel(
    index_ref, weight_ref, slope_ref, theta_out, slope_out,
    index_buf, weight_buf, slope_buf, sems,
):
    band_at = lax.axis_index("band")
    plane = band_at // 2
    copies = [
        pltpu.make_async_copy(index_ref.at[plane], index_buf, sems.at[0]),
        pltpu.make_async_copy(weight_ref.at[:, plane], weight_buf, sems.at[1]),
        pltpu.make_async_copy(slope_ref.at[:, plane], slope_buf, sems.at[2]),
    ]
    for copy in copies:
        copy.start()
    for copy in copies:
        copy.wait()
    parity = band_at % 2
    rel = index_buf[...] - parity * HALF_NA
    fields = [weight_buf[offset] for offset in range(4)]
    for node in range(HALF_NA):
        theta_out[node] = node_sum(rel, fields, node)
    rows = pl.ds(parity, 64, stride=2)
    rel = index_buf[rows, :]
    fields = [slope_buf[offset, rows, :] for offset in range(4)]
    for node in range(NA):
        slope_out[node] = node_sum(rel, fields, node)


def load_kernel(own_ref, phi_far, cas_far, phi_ref, cas_ref, phi_sems, cas_sem):
    copies = [pltpu.make_async_copy(cas_far, cas_ref, cas_sem)]
    copies += [
        pltpu.make_async_copy(phi_far.at[step], phi_ref.at[step], phi_sems.at[step])
        for step in range(NEAR)
    ]
    for copy in copies:
        copy.start()
    for copy in copies:
        copy.wait()


def forward_kernel(own_ref, other_ref, coefficient_ref, cas_ref, out_ref):
    own, other = own_ref[...], other_ref[...]
    first = lax.axis_index("band") % 2 == 0
    density = jnp.concatenate([jnp.where(first, own, other), jnp.where(first, other, own)], axis=0)
    wide, row = cas_ref[: 2 * N], cas_ref[2 * N :]
    theta = density[None] * coefficient_ref[...]
    along_z = rows_times(theta.reshape(HALF_NA * N, N), wide)
    for pair in range(ROWS):
        items = []
        for node in (2 * pair, 2 * pair + 1):
            waves = times_block(row, along_z[node * N : (node + 1) * N])
            items += [waves[slot * 32 : slot * 32 + 32] for slot in range(4)]
        for block, item in enumerate(turned_groups(items)):
            out_ref[pl.ds(block * ROWS + pair, 32, stride=8 * ROWS), :] = item


def mix_kernel(data_ref, cas_ref, twist_ref, phi_ref, far_ref, out_ref, spec_ref, mixed_ref, late_ref, sems):
    cas = cas_ref[...]
    late = [
        pltpu.make_async_copy(far_ref.at[NEAR + step], late_ref.at[step], sems.at[step])
        for step in range(GROUPS - NEAR)
    ]
    for copy in late:
        copy.start()

    def lines(half, pair, at):
        return pl.ds((at * 2 + half) * 16 * ROWS + pair, 16, stride=ROWS)

    for half in range(2):
        for pair in range(ROWS):
            block = jnp.concatenate([data_ref[lines(half, pair, at), :] for at in range(8)], axis=0)
            start = (half * ROWS + pair) * N
            spec_ref[start : start + N, :] = rows_times(block.T, cas)

    def group(step, phi_at):
        spec = [spec_ref[pl.ds(node * POINTS + step * 8, 8), :] for node in range(NA)]
        total = [None] * NA
        item = 0
        for a in range(NA):
            for b in range(a, NA):
                phi = phi_at[item]
                item += 1
                term = phi * spec[a]
                total[b] = term if total[b] is None else total[b] + term
                if a != b:
                    term = phi * spec[b]
                    total[a] = term if total[a] is None else total[a] + term
        for b in range(NA):
            mixed_ref[pl.ds(b * POINTS + step * 8, 8), :] = total[b]

    def near(step, carry):
        group(step, phi_ref.at[step])
        return carry

    def far(step, carry):
        group(NEAR + step, late_ref.at[step])
        return carry

    lax.fori_loop(0, NEAR, near, 0)
    for copy in late:
        copy.wait()
    lax.fori_loop(0, GROUPS - NEAR, far, 0)
    wave_set = lax.axis_index("band") * 2 + lax.axis_index("grid") // 8
    twist = [twist_ref[pl.ds(wave_set * 4 + factor, 1), :] for factor in range(4)]
    for pair in range(ROWS):
        even, odd = [], []
        for node in range(4 * pair, 4 * pair + 4):
            start = node * POINTS
            slots = [mixed_ref[start + 16 * slot : start + 16 * slot + 16, :] for slot in range(4)]
            even += [slots[0] + slots[1], slots[2] + slots[3]]
            near, other = slots[0] - slots[1], slots[2] - slots[3]
            odd += [twist[0] * near + twist[1] * other, twist[2] * near + twist[3] * other]
        for half, rows in enumerate((even, odd)):
            block = times_block_turned(cas, jnp.concatenate(rows, axis=0))
            for at in range(8):
                out_ref[lines(half, pair, at), :] = block[at * 16 : at * 16 + 16]


def inverse_kernel(data_ref, coefficient_ref, cas_ref, half_ref, out_ref):
    cas, row = cas_ref[...], half_ref[...]
    along_y = []
    for pair in range(ROWS):
        items = turned_groups(
            [data_ref[pl.ds(block * ROWS + pair, 32, stride=8 * ROWS), :] for block in range(8)]
        )
        for at in range(4):
            waves = jnp.concatenate([items[2 * at], items[2 * at + 1]], axis=0)
            along_y.append(times_block(row, waves))
    fields = rows_times(jnp.concatenate(along_y, axis=0), cas)
    total = fields[:64] * coefficient_ref[0]
    for node in range(1, NA):
        total = total + fields[node * 64 : (node + 1) * 64] * coefficient_ref[node]
    out_ref[...] = total * (1.0 / float(N) ** 3)


def weave_kernel(data_ref, out_ref, plane_ref, sems):
    copies = []
    for plane in range(8):
        for parity in range(2):
            plane_ref[plane, pl.ds(parity, 64, stride=2), :] = data_ref[2 * plane + parity]
        copies.append(
            pltpu.make_async_copy(plane_ref.at[plane], out_ref.at[plane], sems.at[plane])
        )
        copies[-1].start()
    for copy in copies:
        copy.wait()


def vmem():
    return pl.BlockSpec(memory_space=pltpu.VMEM)


def anywhere():
    return pl.BlockSpec(memory_space=pl.ANY)


def far(value):
    return pltpu.with_memory_space_constraint(value, pltpu.HBM)


def per_device(partial_density, node_index, node_weight, node_slope, kernel_table):
    table = cas_table()
    cas = split_constant(table)
    cas_two = jnp.concatenate([cas, split_row(table[wave_order()])], axis=0)
    x_order = np.arange(N).reshape(16, 8).T.reshape(-1)
    cas_x = split_constant(table[x_order])
    partner = [(i, i ^ 1) for i in range(16)]
    axes = ("band", "grid")
    f32 = jnp.float32

    phi_far = pl.pallas_call(
        phi_kernel,
        out_shape=pltpu.HBM((GROUPS, PAIRS, 8, N), f32),
        in_specs=[vmem()],
        out_specs=anywhere(),
        scratch_shapes=[
            pltpu.VMEM((PAIR_ROWS, N), f32),
            pltpu.VMEM((POINTS, N), jnp.int32),
            pltpu.VMEM((POINTS, N), f32),
            pltpu.VMEM((8 * PAIR_ROWS, N), f32),
            pltpu.VMEM((2, PAIRS, 8, N), f32),
            pltpu.SemaphoreType.DMA((2,)),
        ],
        compiler_params=pltpu.CompilerParams(vmem_limit_bytes=8 << 20),
        cost_estimate=pl.CostEstimate(flops=4 * 10**9, bytes_accessed=8 << 20, transcendentals=0),
        name="phi",
    )(kernel_table)

    theta, slope = pl.pallas_call(
        fields_kernel,
        out_shape=[pltpu.VMEM((HALF_NA, N, N), f32), pltpu.VMEM((NA, 64, N), f32)],
        in_specs=[anywhere()] * 3,
        out_specs=[vmem()] * 2,
        scratch_shapes=[
            pltpu.VMEM((N, N), jnp.int32),
            pltpu.VMEM((4, N, N), f32),
            pltpu.VMEM((4, N, N), f32),
            pltpu.SemaphoreType.DMA((3,)),
        ],
        compiler_params=pltpu.CompilerParams(vmem_limit_bytes=4 << 20),
        cost_estimate=pl.CostEstimate(flops=10**8, bytes_accessed=2 << 20, transcendentals=0),
        name="fields",
    )(far(node_index), far(node_weight), far(node_slope))
    parts = lax.all_to_all(partial_density.reshape(16, 64, N), "band", 0, 0, tiled=True)
    own = jnp.sum(parts, axis=0)
    own, phi_far, slope, theta = lax.optimization_barrier((own, phi_far, slope, theta))
    other = lax.ppermute(own, "band", partner)
    phi, cas_near = pl.pallas_call(
        load_kernel,
        out_shape=[
            pltpu.VMEM((NEAR, PAIRS, 8, N), f32),
            pltpu.VMEM(cas_two.shape, cas_two.dtype),
        ],
        in_specs=[anywhere()] * 3,
        out_specs=[vmem()] * 2,
        scratch_shapes=[pltpu.SemaphoreType.DMA((NEAR,)), pltpu.SemaphoreType.DMA],
        compiler_params=pltpu.CompilerParams(vmem_limit_bytes=2 << 20),
        cost_estimate=pl.CostEstimate(flops=10**9, bytes_accessed=8 << 20, transcendentals=0),
        name="load",
    )(own, far(phi_far), far(cas_two))
    lines = pl.pallas_call(
        forward_kernel,
        out_shape=jax.ShapeDtypeStruct((256 * ROWS, N), f32),
        in_specs=[vmem()] * 4,
        out_specs=vmem(),
        compiler_params=pltpu.CompilerParams(vmem_limit_bytes=12 << 20),
        name="forward",
    )(own, other, theta, cas_near)
    lines = lax.all_to_all(lines.reshape(256, 1, ROWS * N), axes, 0, 0, tiled=True)
    lines = lines.reshape(256 * ROWS, N)
    lines = pl.pallas_call(
        mix_kernel,
        out_shape=jax.ShapeDtypeStruct((256 * ROWS, N), f32),
        in_specs=[vmem()] * 4 + [anywhere()],
        out_specs=vmem(),
        scratch_shapes=[
            pltpu.VMEM((NA * POINTS, N), f32),
            pltpu.VMEM((NA * POINTS, N), f32),
            pltpu.VMEM((GROUPS - NEAR, PAIRS, 8, N), f32),
            pltpu.SemaphoreType.DMA((GROUPS - NEAR,)),
        ],
        compiler_params=pltpu.CompilerParams(vmem_limit_bytes=24 << 20),
        name="mix",
    )(lines, cas_x, twist_table(), phi, far(phi_far))
    lines = lax.all_to_all(lines.reshape(256, 1, ROWS * N), axes, 0, 0, tiled=True)
    lines = lines.reshape(256 * ROWS, N)
    share = pl.pallas_call(
        inverse_kernel,
        out_shape=jax.ShapeDtypeStruct((64, N), f32),
        in_specs=[vmem()] * 4,
        out_specs=vmem(),
        compiler_params=pltpu.CompilerParams(vmem_limit_bytes=12 << 20),
        name="inverse",
    )(lines, slope, cas, split_row(half_table()))
    gathered = lax.all_to_all(
        jnp.broadcast_to(share[None], (16, 64, N)), "band", 0, 0, tiled=True
    )
    return pl.pallas_call(
        weave_kernel,
        out_shape=pltpu.HBM((8, N, N), f32),
        in_specs=[vmem()],
        out_specs=anywhere(),
        scratch_shapes=[pltpu.VMEM((8, N, N), f32), pltpu.SemaphoreType.DMA((8,))],
        compiler_params=pltpu.CompilerParams(vmem_limit_bytes=4 << 20),
        name="weave",
    )(gathered)


def solution(mesh):
    placed = (
        P("band", "grid", None, None),
        P("grid", None, None),
        P(None, "grid", None, None),
        P(None, "grid", None, None),
        P(),
    )
    return jax.shard_map(
        per_device, mesh=mesh, in_specs=placed, out_specs=P("grid", None, None), check_vma=False
    )
```

```python
import jax
import jax.numpy as jnp
import numpy as np
from jax import lax
from jax.experimental import pallas as pl
from jax.experimental.pallas import tpu as pltpu
from jax.sharding import PartitionSpec as P

N = 128
NA = 20
PAIRS = NA * (NA + 1) // 2
PAIR_ROWS = 216
POINTS = 64
ROWS = 5
GROUPS = 6
PHI_POINTS = 8 * GROUPS


def cas_table():
    idx = np.arange(N)
    angle = 2.0 * np.pi * ((idx[:, None] * idx[None, :]) % N) / N
    return np.cos(angle) + np.sin(angle)


def wave_order():
    sets = np.arange(32)
    other = np.where(sets == 0, 32, 64 - sets)
    return np.concatenate([sets, sets + 64, other, other + 64])


def half_table():
    idx = np.arange(64)
    order = wave_order().reshape(4, 32)[[0, 2]].reshape(-1)
    angle = 2.0 * np.pi * ((idx[:, None] * order[None, :]) % 64) / 64
    return np.cos(angle) + np.sin(angle)


def twist_table():
    angle = np.pi * np.arange(32) / 64
    factors = np.stack([np.cos(angle), np.sin(angle), np.sin(angle), -np.cos(angle)], axis=1)
    factors[0] = (1.0, 0.0, 0.0, 1.0)
    return jnp.asarray(np.repeat(factors.reshape(-1, 1), N, axis=1), jnp.float32)


def split_row(table):
    high = jnp.asarray(table, jnp.float32).astype(jnp.bfloat16)
    low = (jnp.asarray(table, jnp.float32) - high.astype(jnp.float32)).astype(jnp.bfloat16)
    return jnp.concatenate([high, low], axis=1)


def split_constant(table):
    row = split_row(table)
    return jnp.concatenate([row, row], axis=0)


def split_value(value):
    high = value.astype(jnp.bfloat16)
    low = (value - high.astype(jnp.float32)).astype(jnp.bfloat16)
    return high, low


def product(left, right, dims=((1,), (0,))):
    dot = lambda a, b: lax.dot_general(a, b, (dims, ((), ())), preferred_element_type=jnp.float32)
    return dot(left[0], right[0]) + (dot(left[0], right[1]) + dot(left[1], right[0]))


def halves_added(value):
    return value[:, :N] + value[:, N:]


def rows_times(value, wide):
    parts = jnp.concatenate(split_value(value), axis=1)
    return halves_added(jnp.dot(parts, wide, preferred_element_type=jnp.float32))


def times_block(row, value):
    parts = jnp.concatenate(split_value(value), axis=1)
    parts = jnp.concatenate([parts, parts], axis=0)
    return halves_added(jnp.dot(row, parts, preferred_element_type=jnp.float32))


def times_block_turned(wide, value):
    parts = jnp.concatenate(split_value(value), axis=0)
    parts = jnp.concatenate([parts, parts], axis=1)
    dims = (((1,), (1,)), ((), ()))
    return halves_added(
        lax.dot_general(wide[:N], parts, dims, preferred_element_type=jnp.float32)
    )


def turned_groups(items):
    items = list(items)
    group = lax.broadcasted_iota(jnp.int32, items[0].shape, 1) // 16
    for bit in (1, 2, 4):
        upper = group // bit % 2 == 1
        for at in range(8):
            if at & bit == 0:
                first, second = items[at], items[at | bit]
                items[at] = jnp.where(upper, pltpu.roll(second, bit * 16, 1), first)
                items[at | bit] = jnp.where(upper, second, pltpu.roll(first, N - bit * 16, 1))
    return items


def node_sum(rel, fields, node):
    out = jnp.zeros_like(fields[0])
    for offset in range(4):
        out = jnp.where(rel == node - (offset - 1), fields[offset], out)
    return out


def frequency(positions):
    return jnp.where(positions < N // 2, positions, positions - N)


def phi_kernel(table_ref, near_ref, out_ref, flat_ref, shell_ref, fraction_ref, stage_ref, group_ref, sems):
    flat_ref[...] = jnp.zeros_like(flat_ref)
    start = 0
    for node in range(NA):
        count = NA - node
        flat_ref[start : start + count, 0 : table_ref.shape[2]] = table_ref[node, node:NA, :]
        start += count
    table = split_value(flat_ref[...])
    band_at, grid_at = lax.axis_index("band"), lax.axis_index("grid")
    wave_set = band_at * 2 + grid_at // 8
    point = lax.broadcasted_iota(jnp.int32, (PHI_POINTS, N), 0)
    slot = point // 16
    other = jnp.where(wave_set == 0, 32, 64 - wave_set)
    freq_y = frequency(jnp.where(slot < 2, wave_set, other) + slot % 2 * 64)
    freq_z = frequency(point % 16 + grid_at % 8 * 16)
    freq_x = frequency(lax.broadcasted_iota(jnp.int32, (PHI_POINTS, N), 1))
    square = freq_x * freq_x + freq_z * freq_z + freq_y * freq_y
    root = jnp.sqrt(square.astype(jnp.float32))
    shell = root.astype(jnp.int32)
    shell = shell - (shell * shell > square).astype(jnp.int32)
    shell = shell + ((shell + 1) * (shell + 1) <= square).astype(jnp.int32)
    shell_ref[...] = shell
    fraction_ref[...] = root - shell.astype(jnp.float32)
    row = lax.broadcasted_iota(jnp.int32, (N, N), 0)

    def weights(at):
        low = shell_ref[pl.ds(at, 1), :]
        part = fraction_ref[pl.ds(at, 1), :]
        return jnp.where(row == low, 1.0 - part, jnp.where(row == low + 1, part, 0.0))

    def put(step):
        slot = step % 2
        return pltpu.make_async_copy(group_ref.at[slot], out_ref.at[step], sems.at[slot])

    def group(step, carry):
        for pair in range(4):
            first = step * 8 + pair * 2
            both = jnp.concatenate([weights(first), weights(first + 1)], axis=1)
            value = product(table, split_value(both))
            stage_ref[pair * 2 * PAIR_ROWS : (pair * 2 + 1) * PAIR_ROWS, :] = value[:, :N]
            stage_ref[(pair * 2 + 1) * PAIR_ROWS : (pair * 2 + 2) * PAIR_ROWS, :] = value[:, N:]

        @pl.when(step >= 2)
        def _():
            put(step - 2).wait()

        for item in range(PAIRS):
            group_ref[step % 2, item] = stage_ref[pl.ds(item, 8, stride=PAIR_ROWS), :]
        put(step).start()

        @pl.when(step < 2)
        def _():
            near_ref[step] = group_ref[step % 2]

        return carry

    lax.fori_loop(0, GROUPS, group, 0)
    put(GROUPS - 2).wait()
    put(GROUPS - 1).wait()


def fields_kernel(
    index_ref, weight_ref, slope_ref, theta_out, slope_out,
    index_buf, weight_buf, slope_buf, sems,
):
    band_at = lax.axis_index("band")
    plane = band_at // 2
    copies = [
        pltpu.make_async_copy(index_ref.at[plane], index_buf, sems.at[0]),
        pltpu.make_async_copy(weight_ref.at[:, plane], weight_buf, sems.at[1]),
        pltpu.make_async_copy(slope_ref.at[:, plane], slope_buf, sems.at[2]),
    ]
    for copy in copies:
        copy.start()
    for copy in copies:
        copy.wait()
    rows = pl.ds(band_at % 2, 64, stride=2)
    rel = index_buf[rows, :]
    for buf, out_ref in ((weight_buf, theta_out), (slope_buf, slope_out)):
        fields = [buf[offset, rows, :] for offset in range(4)]
        for node in range(NA):
            out_ref[node] = node_sum(rel, fields, node)


def sort_kernel(far_ref, out_ref, plane_ref, sorted_ref, in_sems, out_sems):
    def get(plane):
        return pltpu.make_async_copy(far_ref.at[plane], plane_ref.at[plane], in_sems.at[plane])

    def put(plane):
        return pltpu.make_async_copy(
            sorted_ref.at[pl.ds(2 * plane, 2)], out_ref.at[pl.ds(2 * plane, 2)], out_sems.at[plane]
        )

    for plane in range(8):
        get(plane).start()
    for plane in range(8):
        get(plane).wait()
        for parity in range(2):
            sorted_ref[2 * plane + parity] = plane_ref[plane, pl.ds(parity, 64, stride=2), :]
        put(plane).start()
    for plane in range(8):
        put(plane).wait()


def forward_kernel(parts_ref, coefficient_ref, cas_ref, half_ref, far_ref, out_ref, near_ref, sem):
    copy = pltpu.make_async_copy(far_ref.at[2], near_ref, sem)
    copy.start()
    density = parts_ref[0]
    for part in range(1, 16):
        density = density + parts_ref[part]
    row = half_ref[...]
    theta = density[None] * coefficient_ref[...]
    along_z = rows_times(theta.reshape(NA * 64, N), cas_ref[...])
    for pair in range(ROWS):
        items = []
        for node in range(4 * pair, 4 * pair + 4):
            waves = times_block(row, along_z[node * 64 : (node + 1) * 64])
            items += [waves[:32], waves[32:]]
        for block, item in enumerate(turned_groups(items)):
            out_ref[pl.ds(block * ROWS + pair, 32, stride=8 * ROWS), :] = item
    copy.wait()


def mix_kernel(
    data_ref, cas_ref, twist_ref, first_ref, second_ref, far_ref, out_ref,
    spec_ref, mixed_ref, late_ref, sems,
):
    cas = cas_ref[...]
    wave_set = lax.axis_index("band") * 2 + lax.axis_index("grid") // 8
    paired = wave_set != 0
    late = [
        pltpu.make_async_copy(far_ref.at[3 + step], late_ref.at[step], sems.at[step])
        for step in range(3)
    ]
    late[0].start()

    @pl.when(jnp.logical_not(paired))
    def _():
        late[1].start()
        late[2].start()

    twist = [twist_ref[pl.ds(wave_set * 4 + factor, 1), :] for factor in range(4)]

    def lines(half, pair, at):
        return pl.ds((at * 2 + half) * 16 * ROWS + pair, 16, stride=ROWS)

    for pair in range(ROWS):
        even, odd = (
            rows_times(
                jnp.concatenate([data_ref[lines(half, pair, at), :] for at in range(8)], axis=0).T,
                cas,
            )
            for half in range(2)
        )
        for at in range(4):
            start = (4 * pair + at) * POINTS
            near, other = odd[at * 32 : at * 32 + 16], odd[at * 32 + 16 : at * 32 + 32]
            turned = (
                twist[0] * near + twist[1] * other,
                twist[2] * near + twist[3] * other,
            )
            for residue in range(2):
                first = even[at * 32 + 16 * residue : at * 32 + 16 * residue + 16]
                base = start + 32 * residue
                spec_ref[base : base + 16, :] = first + turned[residue]
                spec_ref[base + 16 : base + 32, :] = first - turned[residue]

    def group(step, phi_at):
        spec = [spec_ref[pl.ds(node * POINTS + step * 8, 8), :] for node in range(NA)]
        total = [None] * NA
        item = 0
        for a in range(NA):
            for b in range(a, NA):
                phi = phi_at[item]
                item += 1
                term = phi * spec[a]
                total[b] = term if total[b] is None else total[b] + term
                if a != b:
                    term = phi * spec[b]
                    total[a] = term if total[a] is None else total[a] + term
        for b in range(NA):
            mixed_ref[pl.ds(b * POINTS + step * 8, 8), :] = total[b]

    def each(start, count, gap, phi_of):
        def body(turn, carry):
            group(start + gap * turn, phi_of(turn))
            return carry

        lax.fori_loop(0, count, body, 0)

    each(0, 2, 1, lambda turn: first_ref.at[turn])
    group(2, second_ref)

    @pl.when(paired)
    def _():
        each(6, 2, 1, lambda turn: first_ref.at[turn])
        group(4, second_ref)
        late[0].wait()
        each(3, 2, 2, lambda turn: late_ref.at[0])

    @pl.when(jnp.logical_not(paired))
    def _():
        late[0].wait()
        group(3, late_ref.at[0])
        for step in (1, 2):
            late[step].wait()
            each(3 + step, 2, 2, lambda turn, step=step: late_ref.at[step])

    for pair in range(ROWS):
        even, odd = [], []
        for node in range(4 * pair, 4 * pair + 4):
            start = node * POINTS
            slots = [mixed_ref[start + 16 * slot : start + 16 * slot + 16, :] for slot in range(4)]
            even += [slots[0] + slots[1], slots[2] + slots[3]]
            near, other = slots[0] - slots[1], slots[2] - slots[3]
            odd += [twist[0] * near + twist[1] * other, twist[2] * near + twist[3] * other]
        for half, rows in enumerate((even, odd)):
            block = times_block_turned(cas, jnp.concatenate(rows, axis=0))
            for at in range(8):
                out_ref[lines(half, pair, at), :] = block[at * 16 : at * 16 + 16]


def inverse_kernel(data_ref, coefficient_ref, cas_ref, half_ref, out_ref):
    cas, row = cas_ref[...], half_ref[...]
    along_y = []
    for pair in range(ROWS):
        items = turned_groups(
            [data_ref[pl.ds(block * ROWS + pair, 32, stride=8 * ROWS), :] for block in range(8)]
        )
        for at in range(4):
            waves = jnp.concatenate([items[2 * at], items[2 * at + 1]], axis=0)
            along_y.append(times_block(row, waves))
    fields = rows_times(jnp.concatenate(along_y, axis=0), cas)
    total = fields[:64] * coefficient_ref[0]
    for node in range(1, NA):
        total = total + fields[node * 64 : (node + 1) * 64] * coefficient_ref[node]
    out_ref[...] = total * (1.0 / float(N) ** 3)


def weave_kernel(data_ref, out_ref, plane_ref, sems):
    copies = []
    for plane in range(8):
        for parity in range(2):
            plane_ref[plane, pl.ds(parity, 64, stride=2), :] = data_ref[2 * plane + parity]
        copies.append(
            pltpu.make_async_copy(plane_ref.at[plane], out_ref.at[plane], sems.at[plane])
        )
        copies[-1].start()
    for copy in copies:
        copy.wait()


def vmem():
    return pl.BlockSpec(memory_space=pltpu.VMEM)


def anywhere():
    return pl.BlockSpec(memory_space=pl.ANY)


def far(value):
    return pltpu.with_memory_space_constraint(value, pltpu.HBM)


def per_device(partial_density, node_index, node_weight, node_slope, kernel_table):
    table = cas_table()
    cas = split_constant(table)
    half = half_table()
    x_order = np.arange(N).reshape(16, 8).T.reshape(-1)
    cas_x = split_constant(table[x_order])
    axes = ("band", "grid")
    f32 = jnp.float32

    phi_first, phi_far = pl.pallas_call(
        phi_kernel,
        out_shape=[
            pltpu.VMEM((2, PAIRS, 8, N), f32),
            pltpu.HBM((GROUPS, PAIRS, 8, N), f32),
        ],
        in_specs=[vmem()],
        out_specs=[vmem(), anywhere()],
        scratch_shapes=[
            pltpu.VMEM((PAIR_ROWS, N), f32),
            pltpu.VMEM((PHI_POINTS, N), jnp.int32),
            pltpu.VMEM((PHI_POINTS, N), f32),
            pltpu.VMEM((8 * PAIR_ROWS, N), f32),
            pltpu.VMEM((2, PAIRS, 8, N), f32),
            pltpu.SemaphoreType.DMA((2,)),
        ],
        compiler_params=pltpu.CompilerParams(vmem_limit_bytes=8 << 20),
        cost_estimate=pl.CostEstimate(flops=4 * 10**9, bytes_accessed=8 << 20, transcendentals=0),
        name="phi",
    )(kernel_table)

    theta, slope = pl.pallas_call(
        fields_kernel,
        out_shape=[pltpu.VMEM((NA, 64, N), f32), pltpu.HBM((NA, 64, N), f32)],
        in_specs=[anywhere()] * 3,
        out_specs=[vmem()] * 2,
        scratch_shapes=[
            pltpu.VMEM((N, N), jnp.int32),
            pltpu.VMEM((4, N, N), f32),
            pltpu.VMEM((4, N, N), f32),
            pltpu.SemaphoreType.DMA((3,)),
        ],
        compiler_params=pltpu.CompilerParams(vmem_limit_bytes=4 << 20),
        cost_estimate=pl.CostEstimate(flops=10**8, bytes_accessed=2 << 20, transcendentals=0),
        name="fields",
    )(far(node_index), far(node_weight), far(node_slope))
    rows = pl.pallas_call(
        sort_kernel,
        out_shape=pltpu.HBM((16, 64, N), f32),
        in_specs=[anywhere()],
        out_specs=anywhere(),
        scratch_shapes=[
            pltpu.VMEM((8, N, N), f32),
            pltpu.VMEM((16, 64, N), f32),
            pltpu.SemaphoreType.DMA((8,)),
            pltpu.SemaphoreType.DMA((8,)),
        ],
        compiler_params=pltpu.CompilerParams(vmem_limit_bytes=4 << 20),
        name="sort_rows",
    )(far(partial_density[0]))
    parts = lax.all_to_all(rows, "band", 0, 0, tiled=True)
    parts, phi_first, phi_far, slope, theta = lax.optimization_barrier(
        (parts, phi_first, phi_far, slope, theta)
    )
    lines, phi_second = pl.pallas_call(
        forward_kernel,
        out_shape=[
            jax.ShapeDtypeStruct((256 * ROWS, N), f32),
            pltpu.VMEM((PAIRS, 8, N), f32),
        ],
        in_specs=[vmem()] * 4 + [anywhere()],
        out_specs=[vmem()] * 2,
        scratch_shapes=[pltpu.SemaphoreType.DMA],
        compiler_params=pltpu.CompilerParams(vmem_limit_bytes=12 << 20),
        name="forward",
    )(parts, theta, cas, split_row(half.T), far(phi_far))
    lines = lax.all_to_all(lines.reshape(256, 1, ROWS * N), axes, 0, 0, tiled=True)
    lines = lines.reshape(256 * ROWS, N)
    lines = pl.pallas_call(
        mix_kernel,
        out_shape=jax.ShapeDtypeStruct((256 * ROWS, N), f32),
        in_specs=[vmem()] * 5 + [anywhere()],
        out_specs=vmem(),
        scratch_shapes=[
            pltpu.VMEM((NA * POINTS, N), f32),
            pltpu.VMEM((NA * POINTS, N), f32),
            pltpu.VMEM((3, PAIRS, 8, N), f32),
            pltpu.SemaphoreType.DMA((3,)),
        ],
        compiler_params=pltpu.CompilerParams(vmem_limit_bytes=24 << 20),
        name="mix",
    )(lines, cas_x, twist_table(), phi_first, phi_second, far(phi_far))
    lines = lax.all_to_all(lines.reshape(256, 1, ROWS * N), axes, 0, 0, tiled=True)
    lines = lines.reshape(256 * ROWS, N)
    share = pl.pallas_call(
        inverse_kernel,
        out_shape=jax.ShapeDtypeStruct((64, N), f32),
        in_specs=[vmem()] * 4,
        out_specs=vmem(),
        compiler_params=pltpu.CompilerParams(vmem_limit_bytes=12 << 20),
        name="inverse",
    )(lines, slope, cas, split_row(half))
    gathered = lax.all_to_all(
        jnp.broadcast_to(share[None], (16, 64, N)), "band", 0, 0, tiled=True
    )
    return pl.pallas_call(
        weave_kernel,
        out_shape=pltpu.HBM((8, N, N), f32),
        in_specs=[vmem()],
        out_specs=anywhere(),
        scratch_shapes=[pltpu.VMEM((8, N, N), f32), pltpu.SemaphoreType.DMA((8,))],
        compiler_params=pltpu.CompilerParams(vmem_limit_bytes=4 << 20),
        name="weave",
    )(gathered)


def solution(mesh):
    placed = (
        P("band", "grid", None, None),
        P("grid", None, None),
        P(None, "grid", None, None),
        P(None, "grid", None, None),
        P(),
    )
    return jax.shard_map(
        per_device, mesh=mesh, in_specs=placed, out_specs=P("grid", None, None), check_vma=False
    )
```

```python
import jax
import jax.numpy as jnp
import numpy as np
from jax import lax
from jax.experimental import pallas as pl
from jax.experimental.pallas import tpu as pltpu
from jax.sharding import PartitionSpec as P

N = 128
NA = 20
PAIRS = NA * (NA + 1) // 2
PAIR_ROWS = 216
POINTS = 64
ROWS = 5
GROUPS = 6
PHI_POINTS = 8 * GROUPS


def cas_table():
    idx = np.arange(N)
    angle = 2.0 * np.pi * ((idx[:, None] * idx[None, :]) % N) / N
    return np.cos(angle) + np.sin(angle)


def wave_order():
    sets = np.arange(32)
    other = np.where(sets == 0, 32, 64 - sets)
    return np.concatenate([sets, sets + 64, other, other + 64])


def half_table():
    idx = np.arange(64)
    order = wave_order().reshape(4, 32)[[0, 2]].reshape(-1)
    angle = 2.0 * np.pi * ((idx[:, None] * order[None, :]) % 64) / 64
    return np.cos(angle) + np.sin(angle)


def twist_table():
    angle = np.pi * np.arange(32) / 64
    factors = np.stack([np.cos(angle), np.sin(angle), np.sin(angle), -np.cos(angle)], axis=1)
    factors[0] = (1.0, 0.0, 0.0, 1.0)
    return jnp.asarray(np.repeat(factors.reshape(-1, 1), N, axis=1), jnp.float32)


def split_row(table):
    high = jnp.asarray(table, jnp.float32).astype(jnp.bfloat16)
    low = (jnp.asarray(table, jnp.float32) - high.astype(jnp.float32)).astype(jnp.bfloat16)
    return jnp.concatenate([high, low], axis=1)


def split_constant(table):
    row = split_row(table)
    return jnp.concatenate([row, row], axis=0)


def split_value(value):
    high = value.astype(jnp.bfloat16)
    low = (value - high.astype(jnp.float32)).astype(jnp.bfloat16)
    return high, low


def product(left, right, dims=((1,), (0,))):
    dot = lambda a, b: lax.dot_general(a, b, (dims, ((), ())), preferred_element_type=jnp.float32)
    return dot(left[0], right[0]) + (dot(left[0], right[1]) + dot(left[1], right[0]))


def halves_added(value):
    return value[:, :N] + value[:, N:]


def rows_times(value, wide):
    parts = jnp.concatenate(split_value(value), axis=1)
    return halves_added(jnp.dot(parts, wide, preferred_element_type=jnp.float32))


def times_block(row, value):
    parts = jnp.concatenate(split_value(value), axis=1)
    parts = jnp.concatenate([parts, parts], axis=0)
    return halves_added(jnp.dot(row, parts, preferred_element_type=jnp.float32))


def shifted_groups(items, group):
    for bit in (1, 2, 4):
        moved = group // bit % 2 == 1
        items = [jnp.where(moved, items[(at + bit) % 8], items[at]) for at in range(8)]
    return items


def turned_groups(items):
    group = lax.broadcasted_iota(jnp.int32, items[0].shape, 1) // 16
    items = shifted_groups(items, group)
    items = items[:1] + [pltpu.roll(items[at], at * 16, 1) for at in range(1, 8)]
    items = shifted_groups(items, group)
    return [items[-at % 8] for at in range(8)]


def node_sum(rel, fields, node):
    out = jnp.zeros_like(fields[0])
    for offset in range(4):
        out = jnp.where(rel == node - (offset - 1), fields[offset], out)
    return out


def frequency(positions):
    return jnp.where(positions < N // 2, positions, positions - N)


def phi_kernel(table_ref, near_ref, out_ref, flat_ref, shell_ref, fraction_ref, stage_ref, group_ref, sems):
    flat_ref[...] = jnp.zeros_like(flat_ref)
    start = 0
    for node in range(NA):
        count = NA - node
        flat_ref[start : start + count, 0 : table_ref.shape[2]] = table_ref[node, node:NA, :]
        start += count
    table = split_value(flat_ref[...])
    band_at, grid_at = lax.axis_index("band"), lax.axis_index("grid")
    wave_set = band_at * 2 + grid_at // 8
    point = lax.broadcasted_iota(jnp.int32, (PHI_POINTS, N), 0)
    slot = point // 16
    other = jnp.where(wave_set == 0, 32, 64 - wave_set)
    freq_y = frequency(jnp.where(slot < 2, wave_set, other) + slot % 2 * 64)
    freq_z = frequency(point % 16 + grid_at % 8 * 16)
    freq_x = frequency(lax.broadcasted_iota(jnp.int32, (PHI_POINTS, N), 1))
    square = freq_x * freq_x + freq_z * freq_z + freq_y * freq_y
    root = jnp.sqrt(square.astype(jnp.float32))
    shell = root.astype(jnp.int32)
    shell = shell - (shell * shell > square).astype(jnp.int32)
    shell = shell + ((shell + 1) * (shell + 1) <= square).astype(jnp.int32)
    shell_ref[...] = shell
    fraction_ref[...] = root - shell.astype(jnp.float32)
    row = lax.broadcasted_iota(jnp.int32, (N, N), 0)

    def weights(at):
        low = shell_ref[pl.ds(at, 1), :]
        part = fraction_ref[pl.ds(at, 1), :]
        return jnp.where(row == low, 1.0 - part, jnp.where(row == low + 1, part, 0.0))

    def put(step):
        slot = step % 2
        return pltpu.make_async_copy(group_ref.at[slot], out_ref.at[step], sems.at[slot])

    def group(step, carry):
        for pair in range(4):
            first = step * 8 + pair * 2
            both = jnp.concatenate([weights(first), weights(first + 1)], axis=1)
            value = product(table, split_value(both))
            stage_ref[pair * 2 * PAIR_ROWS : (pair * 2 + 1) * PAIR_ROWS, :] = value[:, :N]
            stage_ref[(pair * 2 + 1) * PAIR_ROWS : (pair * 2 + 2) * PAIR_ROWS, :] = value[:, N:]

        @pl.when(step >= 2)
        def _():
            put(step - 2).wait()

        for item in range(PAIRS):
            group_ref[step % 2, item] = stage_ref[pl.ds(item, 8, stride=PAIR_ROWS), :]
        put(step).start()

        @pl.when(step < 2)
        def _():
            near_ref[step] = group_ref[step % 2]

        return carry

    lax.fori_loop(0, GROUPS, group, 0)
    put(GROUPS - 2).wait()
    put(GROUPS - 1).wait()


def fields_kernel(
    index_ref, weight_ref, slope_ref, theta_out, slope_out,
    index_buf, weight_buf, slope_buf, sems,
):
    band_at = lax.axis_index("band")
    plane = band_at // 2
    copies = [
        pltpu.make_async_copy(index_ref.at[plane], index_buf, sems.at[0]),
        pltpu.make_async_copy(weight_ref.at[:, plane], weight_buf, sems.at[1]),
        pltpu.make_async_copy(slope_ref.at[:, plane], slope_buf, sems.at[2]),
    ]
    for copy in copies:
        copy.start()
    for copy in copies:
        copy.wait()
    rows = pl.ds(band_at % 2, 64, stride=2)
    rel = index_buf[rows, :]
    for buf, out_ref in ((weight_buf, theta_out), (slope_buf, slope_out)):
        fields = [buf[offset, rows, :] for offset in range(4)]
        for node in range(NA):
            out_ref[node] = node_sum(rel, fields, node)


def sort_kernel(far_ref, out_ref, plane_ref, sorted_ref, in_sems, out_sems):
    def get(plane):
        return pltpu.make_async_copy(far_ref.at[plane], plane_ref.at[plane], in_sems.at[plane])

    def put(plane):
        return pltpu.make_async_copy(
            sorted_ref.at[pl.ds(2 * plane, 2)], out_ref.at[pl.ds(2 * plane, 2)], out_sems.at[plane]
        )

    for plane in range(8):
        get(plane).start()
    for plane in range(8):
        get(plane).wait()
        for parity in range(2):
            sorted_ref[2 * plane + parity] = plane_ref[plane, pl.ds(parity, 64, stride=2), :]
        put(plane).start()
    for plane in range(8):
        put(plane).wait()


def forward_kernel(parts_ref, coefficient_ref, cas_ref, half_ref, far_ref, out_ref, near_ref, sems):
    paired = lax.axis_index("band") * 2 + lax.axis_index("grid") // 8 != 0
    copies = [
        pltpu.make_async_copy(far_ref.at[2 + step], near_ref.at[step], sems.at[step])
        for step in range(4)
    ]
    copies[0].start()

    @pl.when(jnp.logical_not(paired))
    def _():
        for copy in copies[1:]:
            copy.start()

    density = parts_ref[0]
    for part in range(1, 16):
        density = density + parts_ref[part]
    row = half_ref[...]
    theta = density[None] * coefficient_ref[...]
    along_z = rows_times(theta.reshape(NA * 64, N), cas_ref[...])
    for pair in range(ROWS):
        items = []
        for node in range(4 * pair, 4 * pair + 4):
            waves = times_block(row, along_z[node * 64 : (node + 1) * 64])
            items += [waves[:32], waves[32:]]
        for block, item in enumerate(turned_groups(items)):
            out_ref[pl.ds(block * ROWS + pair, 32, stride=8 * ROWS), :] = item
    copies[0].wait()

    @pl.when(jnp.logical_not(paired))
    def _():
        for copy in copies[1:]:
            copy.wait()


def mix_kernel(
    data_ref, cas_ref, twist_ref, first_ref, second_ref, far_ref, out_ref,
    spec_ref, mixed_ref, late_ref, sem,
):
    cas = cas_ref[...]
    wave_set = lax.axis_index("band") * 2 + lax.axis_index("grid") // 8
    paired = wave_set != 0
    late = pltpu.make_async_copy(far_ref.at[3], late_ref, sem)

    @pl.when(paired)
    def _():
        late.start()

    twist = [twist_ref[pl.ds(wave_set * 4 + factor, 1), :] for factor in range(4)]

    def lines(half, pair, at):
        return pl.ds((at * 2 + half) * 16 * ROWS + pair, 16, stride=ROWS)

    for pair in range(ROWS):
        even, odd = (
            rows_times(
                jnp.concatenate([data_ref[lines(half, pair, at), :] for at in range(8)], axis=0).T,
                cas,
            )
            for half in range(2)
        )
        for at in range(4):
            start = (4 * pair + at) * POINTS
            near, other = odd[at * 32 : at * 32 + 16], odd[at * 32 + 16 : at * 32 + 32]
            turned = (
                twist[0] * near + twist[1] * other,
                twist[2] * near + twist[3] * other,
            )
            for residue in range(2):
                first = even[at * 32 + 16 * residue : at * 32 + 16 * residue + 16]
                base = start + 32 * residue
                spec_ref[base : base + 16, :] = first + turned[residue]
                spec_ref[base + 16 : base + 32, :] = first - turned[residue]

    def group(step, phi_at):
        spec = [spec_ref[pl.ds(node * POINTS + step * 8, 8), :] for node in range(NA)]
        total = [None] * NA
        item = 0
        for a in range(NA):
            for b in range(a, NA):
                phi = phi_at[item]
                item += 1
                term = phi * spec[a]
                total[b] = term if total[b] is None else total[b] + term
                if a != b:
                    term = phi * spec[b]
                    total[a] = term if total[a] is None else total[a] + term
        for b in range(NA):
            mixed_ref[pl.ds(b * POINTS + step * 8, 8), :] = total[b]

    def each(start, count, gap, phi_of):
        def body(turn, carry):
            group(start + gap * turn, phi_of(turn))
            return carry

        lax.fori_loop(0, count, body, 0)

    each(0, 2, 1, lambda turn: first_ref.at[turn])
    group(2, second_ref.at[0])

    @pl.when(paired)
    def _():
        each(6, 2, 1, lambda turn: first_ref.at[turn])
        group(4, second_ref.at[0])
        late.wait()
        each(3, 2, 2, lambda turn: late_ref)

    @pl.when(jnp.logical_not(paired))
    def _():
        group(3, second_ref.at[1])
        each(4, 4, 1, lambda turn: second_ref.at[2 + turn % 2])

    for pair in range(ROWS):
        even, odd = [], []
        for node in range(4 * pair, 4 * pair + 4):
            start = node * POINTS
            slots = [mixed_ref[start + 16 * slot : start + 16 * slot + 16, :] for slot in range(4)]
            even += [slots[0] + slots[1], slots[2] + slots[3]]
            near, other = slots[0] - slots[1], slots[2] - slots[3]
            odd += [twist[0] * near + twist[1] * other, twist[2] * near + twist[3] * other]
        for half, rows in enumerate((even, odd)):
            block = times_block(cas[:N], jnp.concatenate(rows, axis=0).T)
            for at in range(8):
                out_ref[lines(half, pair, at), :] = block[at * 16 : at * 16 + 16]


def inverse_kernel(data_ref, coefficient_ref, cas_ref, half_ref, out_ref):
    cas, row = cas_ref[...], half_ref[...]
    along_y = []
    for pair in range(ROWS):
        items = turned_groups(
            [data_ref[pl.ds(block * ROWS + pair, 32, stride=8 * ROWS), :] for block in range(8)]
        )
        for at in range(4):
            waves = jnp.concatenate([items[2 * at], items[2 * at + 1]], axis=0)
            along_y.append(times_block(row, waves))
    fields = rows_times(jnp.concatenate(along_y, axis=0), cas)
    total = fields[:64] * coefficient_ref[0]
    for node in range(1, NA):
        total = total + fields[node * 64 : (node + 1) * 64] * coefficient_ref[node]
    out_ref[...] = total * (1.0 / float(N) ** 3)


def weave_kernel(data_ref, out_ref, plane_ref, sems):
    copies = []
    for plane in range(8):
        for parity in range(2):
            plane_ref[plane, pl.ds(parity, 64, stride=2), :] = data_ref[2 * plane + parity]
        copies.append(
            pltpu.make_async_copy(plane_ref.at[plane], out_ref.at[plane], sems.at[plane])
        )
        copies[-1].start()
    for copy in copies:
        copy.wait()


def vmem():
    return pl.BlockSpec(memory_space=pltpu.VMEM)


def anywhere():
    return pl.BlockSpec(memory_space=pl.ANY)


def far(value):
    return pltpu.with_memory_space_constraint(value, pltpu.HBM)


def per_device(partial_density, node_index, node_weight, node_slope, kernel_table):
    table = cas_table()
    cas = split_constant(table)
    half = half_table()
    x_order = np.arange(N).reshape(16, 8).T.reshape(-1)
    cas_x = split_constant(table[x_order])
    axes = ("band", "grid")
    f32 = jnp.float32

    phi_first, phi_far = pl.pallas_call(
        phi_kernel,
        out_shape=[
            pltpu.VMEM((2, PAIRS, 8, N), f32),
            pltpu.HBM((GROUPS, PAIRS, 8, N), f32),
        ],
        in_specs=[vmem()],
        out_specs=[vmem(), anywhere()],
        scratch_shapes=[
            pltpu.VMEM((PAIR_ROWS, N), f32),
            pltpu.VMEM((PHI_POINTS, N), jnp.int32),
            pltpu.VMEM((PHI_POINTS, N), f32),
            pltpu.VMEM((8 * PAIR_ROWS, N), f32),
            pltpu.VMEM((2, PAIRS, 8, N), f32),
            pltpu.SemaphoreType.DMA((2,)),
        ],
        compiler_params=pltpu.CompilerParams(vmem_limit_bytes=8 << 20),
        cost_estimate=pl.CostEstimate(flops=4 * 10**9, bytes_accessed=8 << 20, transcendentals=0),
        name="phi",
    )(kernel_table)

    theta, slope = pl.pallas_call(
        fields_kernel,
        out_shape=[pltpu.VMEM((NA, 64, N), f32), pltpu.HBM((NA, 64, N), f32)],
        in_specs=[anywhere()] * 3,
        out_specs=[vmem()] * 2,
        scratch_shapes=[
            pltpu.VMEM((N, N), jnp.int32),
            pltpu.VMEM((4, N, N), f32),
            pltpu.VMEM((4, N, N), f32),
            pltpu.SemaphoreType.DMA((3,)),
        ],
        compiler_params=pltpu.CompilerParams(vmem_limit_bytes=4 << 20),
        cost_estimate=pl.CostEstimate(flops=10**8, bytes_accessed=2 << 20, transcendentals=0),
        name="fields",
    )(far(node_index), far(node_weight), far(node_slope))
    rows = pl.pallas_call(
        sort_kernel,
        out_shape=pltpu.HBM((16, 64, N), f32),
        in_specs=[anywhere()],
        out_specs=anywhere(),
        scratch_shapes=[
            pltpu.VMEM((8, N, N), f32),
            pltpu.VMEM((16, 64, N), f32),
            pltpu.SemaphoreType.DMA((8,)),
            pltpu.SemaphoreType.DMA((8,)),
        ],
        compiler_params=pltpu.CompilerParams(vmem_limit_bytes=4 << 20),
        name="sort_rows",
    )(far(partial_density[0]))
    parts = lax.all_to_all(rows, "band", 0, 0, tiled=True)
    parts, phi_first, phi_far, slope, theta = lax.optimization_barrier(
        (parts, phi_first, phi_far, slope, theta)
    )
    lines, phi_second = pl.pallas_call(
        forward_kernel,
        out_shape=[
            jax.ShapeDtypeStruct((256 * ROWS, N), f32),
            pltpu.VMEM((4, PAIRS, 8, N), f32),
        ],
        in_specs=[vmem()] * 4 + [anywhere()],
        out_specs=[vmem()] * 2,
        scratch_shapes=[pltpu.SemaphoreType.DMA((4,))],
        compiler_params=pltpu.CompilerParams(vmem_limit_bytes=12 << 20),
        name="forward",
    )(parts, theta, cas, split_row(half.T), far(phi_far))
    lines = lax.all_to_all(lines.reshape(256, 1, ROWS * N), axes, 0, 0, tiled=True)
    lines = lines.reshape(256 * ROWS, N)
    lines = pl.pallas_call(
        mix_kernel,
        out_shape=jax.ShapeDtypeStruct((256 * ROWS, N), f32),
        in_specs=[vmem()] * 5 + [anywhere()],
        out_specs=vmem(),
        scratch_shapes=[
            pltpu.VMEM((NA * POINTS, N), f32),
            pltpu.VMEM((NA * POINTS, N), f32),
            pltpu.VMEM((PAIRS, 8, N), f32),
            pltpu.SemaphoreType.DMA,
        ],
        compiler_params=pltpu.CompilerParams(vmem_limit_bytes=24 << 20),
        name="mix",
    )(lines, cas_x, twist_table(), phi_first, phi_second, far(phi_far))
    lines = lax.all_to_all(lines.reshape(256, 1, ROWS * N), axes, 0, 0, tiled=True)
    lines = lines.reshape(256 * ROWS, N)
    share = pl.pallas_call(
        inverse_kernel,
        out_shape=jax.ShapeDtypeStruct((64, N), f32),
        in_specs=[vmem()] * 4,
        out_specs=vmem(),
        compiler_params=pltpu.CompilerParams(vmem_limit_bytes=12 << 20),
        name="inverse",
    )(lines, slope, cas, split_row(half))
    gathered = lax.all_to_all(
        jnp.broadcast_to(share[None], (16, 64, N)), "band", 0, 0, tiled=True
    )
    return pl.pallas_call(
        weave_kernel,
        out_shape=pltpu.HBM((8, N, N), f32),
        in_specs=[vmem()],
        out_specs=anywhere(),
        scratch_shapes=[pltpu.VMEM((8, N, N), f32), pltpu.SemaphoreType.DMA((8,))],
        compiler_params=pltpu.CompilerParams(vmem_limit_bytes=4 << 20),
        name="weave",
    )(gathered)


def solution(mesh):
    placed = (
        P("band", "grid", None, None),
        P("grid", None, None),
        P(None, "grid", None, None),
        P(None, "grid", None, None),
        P(),
    )
    return jax.shard_map(
        per_device, mesh=mesh, in_specs=placed, out_specs=P("grid", None, None), check_vma=False
    )
```

```python
import jax
import jax.numpy as jnp
import numpy as np
from jax import lax
from jax.experimental import pallas as pl
from jax.experimental.pallas import tpu as pltpu
from jax.sharding import PartitionSpec as P

N = 128
NA = 20
PAIRS = NA * (NA + 1) // 2
PAIR_ROWS = 216
POINTS = 64
ROWS = 5
GROUPS = 6
PHI_POINTS = 8 * GROUPS


def cas_table():
    idx = np.arange(N)
    angle = 2.0 * np.pi * ((idx[:, None] * idx[None, :]) % N) / N
    return np.cos(angle) + np.sin(angle)


def wave_order():
    sets = np.arange(32)
    other = np.where(sets == 0, 32, 64 - sets)
    return np.concatenate([sets, sets + 64, other, other + 64])


def half_table():
    idx = np.arange(64)
    order = wave_order().reshape(4, 32)[[0, 2]].reshape(-1)
    angle = 2.0 * np.pi * ((idx[:, None] * order[None, :]) % 64) / 64
    return np.cos(angle) + np.sin(angle)


def twist_table():
    angle = np.pi * np.arange(32) / 64
    factors = np.stack([np.cos(angle), np.sin(angle), np.sin(angle), -np.cos(angle)], axis=1)
    factors[0] = (1.0, 0.0, 0.0, 1.0)
    return jnp.asarray(np.repeat(factors.reshape(-1, 1), N, axis=1), jnp.float32)


def split_row(table):
    high = jnp.asarray(table, jnp.float32).astype(jnp.bfloat16)
    low = (jnp.asarray(table, jnp.float32) - high.astype(jnp.float32)).astype(jnp.bfloat16)
    return jnp.concatenate([high, low], axis=1)


def split_constant(table):
    row = split_row(table)
    return jnp.concatenate([row, row], axis=0)


def split_value(value):
    high = value.astype(jnp.bfloat16)
    low = (value - high.astype(jnp.float32)).astype(jnp.bfloat16)
    return high, low


def product(left, right, dims=((1,), (0,))):
    dot = lambda a, b: lax.dot_general(a, b, (dims, ((), ())), preferred_element_type=jnp.float32)
    return dot(left[0], right[0]) + (dot(left[0], right[1]) + dot(left[1], right[0]))


def halves_added(value):
    return value[:, :N] + value[:, N:]


def rows_times(value, wide):
    parts = jnp.concatenate(split_value(value), axis=1)
    return halves_added(jnp.dot(parts, wide, preferred_element_type=jnp.float32))


def times_block(row, value):
    parts = jnp.concatenate(split_value(value), axis=1)
    parts = jnp.concatenate([parts, parts], axis=0)
    return halves_added(jnp.dot(row, parts, preferred_element_type=jnp.float32))


def shifted_groups(items, group):
    for bit in (1, 2, 4):
        moved = group // bit % 2 == 1
        items = [jnp.where(moved, items[(at + bit) % 8], items[at]) for at in range(8)]
    return items


def turned_groups(items):
    group = lax.broadcasted_iota(jnp.int32, items[0].shape, 1) // 16
    items = shifted_groups(items, group)
    items = items[:1] + [pltpu.roll(items[at], at * 16, 1) for at in range(1, 8)]
    items = shifted_groups(items, group)
    return [items[-at % 8] for at in range(8)]


def node_sum(rel, fields, node):
    out = jnp.zeros_like(fields[0])
    for offset in range(4):
        out = jnp.where(rel == node - (offset - 1), fields[offset], out)
    return out


def frequency(positions):
    return jnp.where(positions < N // 2, positions, positions - N)


def phi_kernel(table_ref, near_ref, out_ref, flat_ref, shell_ref, fraction_ref, stage_ref, group_ref, sems):
    flat_ref[...] = jnp.zeros_like(flat_ref)
    start = 0
    for node in range(NA):
        count = NA - node
        flat_ref[start : start + count, 0 : table_ref.shape[2]] = table_ref[node, node:NA, :]
        start += count
    table = split_value(flat_ref[...])
    band_at, grid_at = lax.axis_index("band"), lax.axis_index("grid")
    wave_set = band_at * 2 + grid_at // 8
    point = lax.broadcasted_iota(jnp.int32, (PHI_POINTS, N), 0)
    slot = point // 16
    other = jnp.where(wave_set == 0, 32, 64 - wave_set)
    freq_y = frequency(jnp.where(slot < 2, wave_set, other) + slot % 2 * 64)
    freq_z = frequency(point % 16 + grid_at % 8 * 16)
    freq_x = frequency(lax.broadcasted_iota(jnp.int32, (PHI_POINTS, N), 1))
    square = freq_x * freq_x + freq_z * freq_z + freq_y * freq_y
    root = jnp.sqrt(square.astype(jnp.float32))
    shell = root.astype(jnp.int32)
    shell = shell - (shell * shell > square).astype(jnp.int32)
    shell = shell + ((shell + 1) * (shell + 1) <= square).astype(jnp.int32)
    shell_ref[...] = shell
    fraction_ref[...] = root - shell.astype(jnp.float32)
    row = lax.broadcasted_iota(jnp.int32, (N, N), 0)

    def weights(at):
        low = shell_ref[pl.ds(at, 1), :]
        part = fraction_ref[pl.ds(at, 1), :]
        return jnp.where(row == low, 1.0 - part, jnp.where(row == low + 1, part, 0.0))

    def put(step):
        slot = step % 2
        return pltpu.make_async_copy(group_ref.at[slot], out_ref.at[step], sems.at[slot])

    def group(step, carry):
        for pair in range(4):
            first = step * 8 + pair * 2
            both = jnp.concatenate([weights(first), weights(first + 1)], axis=1)
            value = product(table, split_value(both))
            stage_ref[pair * 2 * PAIR_ROWS : (pair * 2 + 1) * PAIR_ROWS, :] = value[:, :N]
            stage_ref[(pair * 2 + 1) * PAIR_ROWS : (pair * 2 + 2) * PAIR_ROWS, :] = value[:, N:]

        @pl.when(step >= 2)
        def _():
            put(step - 2).wait()

        for item in range(PAIRS):
            group_ref[step % 2, item] = stage_ref[pl.ds(item, 8, stride=PAIR_ROWS), :]
        put(step).start()

        @pl.when(step < 2)
        def _():
            near_ref[step] = group_ref[step % 2]

        return carry

    lax.fori_loop(0, GROUPS, group, 0)
    put(GROUPS - 2).wait()
    put(GROUPS - 1).wait()


def fields_kernel(
    index_ref, weight_ref, slope_ref, theta_out, slope_out,
    index_buf, weight_buf, slope_buf, sems,
):
    band_at = lax.axis_index("band")
    plane = band_at // 2
    copies = [
        pltpu.make_async_copy(index_ref.at[plane], index_buf, sems.at[0]),
        pltpu.make_async_copy(weight_ref.at[:, plane], weight_buf, sems.at[1]),
        pltpu.make_async_copy(slope_ref.at[:, plane], slope_buf, sems.at[2]),
    ]
    for copy in copies:
        copy.start()
    for copy in copies:
        copy.wait()
    rows = pl.ds(band_at % 2, 64, stride=2)
    rel = index_buf[rows, :]
    for buf, out_ref in ((weight_buf, theta_out), (slope_buf, slope_out)):
        fields = [buf[offset, rows, :] for offset in range(4)]
        for node in range(NA):
            out_ref[node] = node_sum(rel, fields, node)


def sort_kernel(far_ref, out_ref, plane_ref, sorted_ref, in_sems, out_sems):
    def get(plane):
        return pltpu.make_async_copy(far_ref.at[plane], plane_ref.at[plane], in_sems.at[plane])

    def put(plane):
        return pltpu.make_async_copy(
            sorted_ref.at[pl.ds(2 * plane, 2)], out_ref.at[pl.ds(2 * plane, 2)], out_sems.at[plane]
        )

    for plane in range(8):
        get(plane).start()
    for plane in range(8):
        get(plane).wait()
        for parity in range(2):
            sorted_ref[2 * plane + parity] = plane_ref[plane, pl.ds(parity, 64, stride=2), :]
        put(plane).start()
    for plane in range(8):
        put(plane).wait()


def forward_kernel(parts_ref, coefficient_ref, cas_ref, half_ref, far_ref, out_ref, near_ref, sems):
    paired = lax.axis_index("band") * 2 + lax.axis_index("grid") // 8 != 0
    copies = [
        pltpu.make_async_copy(far_ref.at[2 + step], near_ref.at[step], sems.at[step])
        for step in range(4)
    ]

    @pl.when(jnp.logical_not(paired))
    def _():
        for copy in copies:
            copy.start()

    density = parts_ref[0]
    for part in range(1, 16):
        density = density + parts_ref[part]
    row = half_ref[...]
    theta = density[None] * coefficient_ref[...]
    along_z = rows_times(theta.reshape(NA * 64, N), cas_ref[...])
    for pair in range(ROWS):
        items = []
        for node in range(4 * pair, 4 * pair + 4):
            waves = times_block(row, along_z[node * 64 : (node + 1) * 64])
            items += [waves[:32], waves[32:]]
        for block, item in enumerate(turned_groups(items)):
            out_ref[pl.ds(block * ROWS + pair, 32, stride=8 * ROWS), :] = item

    @pl.when(jnp.logical_not(paired))
    def _():
        for copy in copies:
            copy.wait()


def mix_kernel(
    data_ref, cas_ref, twist_ref, first_ref, second_ref, far_ref, out_ref,
    spec_ref, mixed_ref, late_ref, sems,
):
    cas = cas_ref[...]
    wave_set = lax.axis_index("band") * 2 + lax.axis_index("grid") // 8
    paired = wave_set != 0
    late = [
        pltpu.make_async_copy(far_ref.at[2 + step], late_ref.at[step], sems.at[step])
        for step in range(2)
    ]

    @pl.when(paired)
    def _():
        for copy in late:
            copy.start()

    twist = [twist_ref[pl.ds(wave_set * 4 + factor, 1), :] for factor in range(4)]

    def lines(half, pair, at):
        return pl.ds((at * 2 + half) * 16 * ROWS + pair, 16, stride=ROWS)

    for pair in range(ROWS):
        even, odd = (
            rows_times(
                jnp.concatenate([data_ref[lines(half, pair, at), :] for at in range(8)], axis=0).T,
                cas,
            )
            for half in range(2)
        )
        for at in range(4):
            start = (4 * pair + at) * POINTS
            near, other = odd[at * 32 : at * 32 + 16], odd[at * 32 + 16 : at * 32 + 32]
            turned = (
                twist[0] * near + twist[1] * other,
                twist[2] * near + twist[3] * other,
            )
            for residue in range(2):
                first = even[at * 32 + 16 * residue : at * 32 + 16 * residue + 16]
                base = start + 32 * residue
                spec_ref[base : base + 16, :] = first + turned[residue]
                spec_ref[base + 16 : base + 32, :] = first - turned[residue]

    def group(step, phi_at):
        spec = [spec_ref[pl.ds(node * POINTS + step * 8, 8), :] for node in range(NA)]
        total = [None] * NA
        item = 0
        for a in range(NA):
            for b in range(a, NA):
                phi = phi_at[item]
                item += 1
                term = phi * spec[a]
                total[b] = term if total[b] is None else total[b] + term
                if a != b:
                    term = phi * spec[b]
                    total[a] = term if total[a] is None else total[a] + term
        for b in range(NA):
            mixed_ref[pl.ds(b * POINTS + step * 8, 8), :] = total[b]

    def each(start, count, gap, phi_of):
        def body(turn, carry):
            group(start + gap * turn, phi_of(turn))
            return carry

        lax.fori_loop(0, count, body, 0)

    each(0, 2, 1, lambda turn: first_ref.at[turn])

    @pl.when(paired)
    def _():
        each(6, 2, 1, lambda turn: first_ref.at[turn])
        for step in range(2):
            late[step].wait()
            each(2 + step, 2, 2, lambda turn, step=step: late_ref.at[step])

    @pl.when(jnp.logical_not(paired))
    def _():
        each(2, 2, 1, lambda turn: second_ref.at[turn])
        each(4, 4, 1, lambda turn: second_ref.at[2 + turn % 2])

    for pair in range(ROWS):
        even, odd = [], []
        for node in range(4 * pair, 4 * pair + 4):
            start = node * POINTS
            slots = [mixed_ref[start + 16 * slot : start + 16 * slot + 16, :] for slot in range(4)]
            even += [slots[0] + slots[1], slots[2] + slots[3]]
            near, other = slots[0] - slots[1], slots[2] - slots[3]
            odd += [twist[0] * near + twist[1] * other, twist[2] * near + twist[3] * other]
        for half, rows in enumerate((even, odd)):
            block = times_block(cas[:N], jnp.concatenate(rows, axis=0).T)
            for at in range(8):
                out_ref[lines(half, pair, at), :] = block[at * 16 : at * 16 + 16]


def inverse_kernel(data_ref, coefficient_ref, cas_ref, half_ref, out_ref):
    cas, row = cas_ref[...], half_ref[...]
    along_y = []
    for pair in range(ROWS):
        items = turned_groups(
            [data_ref[pl.ds(block * ROWS + pair, 32, stride=8 * ROWS), :] for block in range(8)]
        )
        for at in range(4):
            waves = jnp.concatenate([items[2 * at], items[2 * at + 1]], axis=0)
            along_y.append(times_block(row, waves))
    fields = rows_times(jnp.concatenate(along_y, axis=0), cas)
    total = fields[:64] * coefficient_ref[0]
    for node in range(1, NA):
        total = total + fields[node * 64 : (node + 1) * 64] * coefficient_ref[node]
    out_ref[...] = total * (1.0 / float(N) ** 3)


def weave_kernel(data_ref, out_ref, plane_ref, sems):
    copies = []
    for plane in range(8):
        for parity in range(2):
            plane_ref[plane, pl.ds(parity, 64, stride=2), :] = data_ref[2 * plane + parity]
        copies.append(
            pltpu.make_async_copy(plane_ref.at[plane], out_ref.at[plane], sems.at[plane])
        )
        copies[-1].start()
    for copy in copies:
        copy.wait()


def vmem():
    return pl.BlockSpec(memory_space=pltpu.VMEM)


def anywhere():
    return pl.BlockSpec(memory_space=pl.ANY)


def far(value):
    return pltpu.with_memory_space_constraint(value, pltpu.HBM)


def per_device(partial_density, node_index, node_weight, node_slope, kernel_table):
    table = cas_table()
    cas = split_constant(table)
    half = half_table()
    x_order = np.arange(N).reshape(16, 8).T.reshape(-1)
    cas_x = split_constant(table[x_order])
    axes = ("band", "grid")
    f32 = jnp.float32

    phi_first, phi_far = pl.pallas_call(
        phi_kernel,
        out_shape=[
            pltpu.VMEM((2, PAIRS, 8, N), f32),
            pltpu.HBM((GROUPS, PAIRS, 8, N), f32),
        ],
        in_specs=[vmem()],
        out_specs=[vmem(), anywhere()],
        scratch_shapes=[
            pltpu.VMEM((PAIR_ROWS, N), f32),
            pltpu.VMEM((PHI_POINTS, N), jnp.int32),
            pltpu.VMEM((PHI_POINTS, N), f32),
            pltpu.VMEM((8 * PAIR_ROWS, N), f32),
            pltpu.VMEM((2, PAIRS, 8, N), f32),
            pltpu.SemaphoreType.DMA((2,)),
        ],
        compiler_params=pltpu.CompilerParams(vmem_limit_bytes=8 << 20),
        cost_estimate=pl.CostEstimate(flops=4 * 10**9, bytes_accessed=8 << 20, transcendentals=0),
        name="phi",
    )(kernel_table)

    theta, slope = pl.pallas_call(
        fields_kernel,
        out_shape=[pltpu.VMEM((NA, 64, N), f32), pltpu.HBM((NA, 64, N), f32)],
        in_specs=[anywhere()] * 3,
        out_specs=[vmem()] * 2,
        scratch_shapes=[
            pltpu.VMEM((N, N), jnp.int32),
            pltpu.VMEM((4, N, N), f32),
            pltpu.VMEM((4, N, N), f32),
            pltpu.SemaphoreType.DMA((3,)),
        ],
        compiler_params=pltpu.CompilerParams(vmem_limit_bytes=4 << 20),
        cost_estimate=pl.CostEstimate(flops=10**8, bytes_accessed=2 << 20, transcendentals=0),
        name="fields",
    )(far(node_index), far(node_weight), far(node_slope))
    rows = pl.pallas_call(
        sort_kernel,
        out_shape=pltpu.HBM((16, 64, N), f32),
        in_specs=[anywhere()],
        out_specs=anywhere(),
        scratch_shapes=[
            pltpu.VMEM((8, N, N), f32),
            pltpu.VMEM((16, 64, N), f32),
            pltpu.SemaphoreType.DMA((8,)),
            pltpu.SemaphoreType.DMA((8,)),
        ],
        compiler_params=pltpu.CompilerParams(vmem_limit_bytes=4 << 20),
        name="sort_rows",
    )(far(partial_density[0]))
    parts = lax.all_to_all(rows, "band", 0, 0, tiled=True)
    parts, phi_first, phi_far, slope, theta = lax.optimization_barrier(
        (parts, phi_first, phi_far, slope, theta)
    )
    lines, phi_second = pl.pallas_call(
        forward_kernel,
        out_shape=[
            jax.ShapeDtypeStruct((256 * ROWS, N), f32),
            pltpu.VMEM((4, PAIRS, 8, N), f32),
        ],
        in_specs=[vmem()] * 4 + [anywhere()],
        out_specs=[vmem()] * 2,
        scratch_shapes=[pltpu.SemaphoreType.DMA((4,))],
        compiler_params=pltpu.CompilerParams(vmem_limit_bytes=12 << 20),
        name="forward",
    )(parts, theta, cas, split_row(half.T), far(phi_far))
    lines = lax.all_to_all(lines.reshape(256, 1, ROWS * N), axes, 0, 0, tiled=True)
    lines = lines.reshape(256 * ROWS, N)
    lines = pl.pallas_call(
        mix_kernel,
        out_shape=jax.ShapeDtypeStruct((256 * ROWS, N), f32),
        in_specs=[vmem()] * 5 + [anywhere()],
        out_specs=vmem(),
        scratch_shapes=[
            pltpu.VMEM((NA * POINTS, N), f32),
            pltpu.VMEM((NA * POINTS, N), f32),
            pltpu.VMEM((2, PAIRS, 8, N), f32),
            pltpu.SemaphoreType.DMA((2,)),
        ],
        compiler_params=pltpu.CompilerParams(vmem_limit_bytes=24 << 20),
        name="mix",
    )(lines, cas_x, twist_table(), phi_first, phi_second, far(phi_far))
    lines = lax.all_to_all(lines.reshape(256, 1, ROWS * N), axes, 0, 0, tiled=True)
    lines = lines.reshape(256 * ROWS, N)
    share = pl.pallas_call(
        inverse_kernel,
        out_shape=jax.ShapeDtypeStruct((64, N), f32),
        in_specs=[vmem()] * 4,
        out_specs=vmem(),
        compiler_params=pltpu.CompilerParams(vmem_limit_bytes=12 << 20),
        name="inverse",
    )(lines, slope, cas, split_row(half))
    gathered = lax.all_to_all(
        jnp.broadcast_to(share[None], (16, 64, N)), "band", 0, 0, tiled=True
    )
    return pl.pallas_call(
        weave_kernel,
        out_shape=pltpu.HBM((8, N, N), f32),
        in_specs=[vmem()],
        out_specs=anywhere(),
        scratch_shapes=[pltpu.VMEM((8, N, N), f32), pltpu.SemaphoreType.DMA((8,))],
        compiler_params=pltpu.CompilerParams(vmem_limit_bytes=4 << 20),
        name="weave",
    )(gathered)


def solution(mesh):
    placed = (
        P("band", "grid", None, None),
        P("grid", None, None),
        P(None, "grid", None, None),
        P(None, "grid", None, None),
        P(),
    )
    return jax.shard_map(
        per_device, mesh=mesh, in_specs=placed, out_specs=P("grid", None, None), check_vma=False
    )
```

```python
import jax
import jax.numpy as jnp
import numpy as np
from jax import lax
from jax.experimental import pallas as pl
from jax.experimental.pallas import tpu as pltpu
from jax.sharding import PartitionSpec as P

N = 128
NA = 20
PAIRS = NA * (NA + 1) // 2
PAIR_ROWS = 216
POINTS = 64
ROWS = 5
GROUPS = 6
PHI_POINTS = 8 * GROUPS


def cas_table():
    idx = np.arange(N)
    angle = 2.0 * np.pi * ((idx[:, None] * idx[None, :]) % N) / N
    return np.cos(angle) + np.sin(angle)


def wave_order():
    sets = np.arange(32)
    other = np.where(sets == 0, 32, 64 - sets)
    return np.concatenate([sets, sets + 64, other, other + 64])


def half_table():
    idx = np.arange(64)
    order = wave_order().reshape(4, 32)[[0, 2]].reshape(-1)
    angle = 2.0 * np.pi * ((idx[:, None] * order[None, :]) % 64) / 64
    return np.cos(angle) + np.sin(angle)


def twist_table():
    angle = np.pi * np.arange(32) / 64
    factors = np.stack([np.cos(angle), np.sin(angle), np.sin(angle), -np.cos(angle)], axis=1)
    factors[0] = (1.0, 0.0, 0.0, 1.0)
    return jnp.asarray(np.repeat(factors.reshape(-1, 1), N, axis=1), jnp.float32)


def split_row(table):
    high = jnp.asarray(table, jnp.float32).astype(jnp.bfloat16)
    low = (jnp.asarray(table, jnp.float32) - high.astype(jnp.float32)).astype(jnp.bfloat16)
    return jnp.concatenate([high, low], axis=1)


def split_constant(table):
    row = split_row(table)
    return jnp.concatenate([row, row], axis=0)


def split_value(value):
    high = value.astype(jnp.bfloat16)
    low = (value - high.astype(jnp.float32)).astype(jnp.bfloat16)
    return high, low


def product(left, right, dims=((1,), (0,))):
    dot = lambda a, b: lax.dot_general(a, b, (dims, ((), ())), preferred_element_type=jnp.float32)
    return dot(left[0], right[0]) + (dot(left[0], right[1]) + dot(left[1], right[0]))


def halves_added(value):
    return value[:, :N] + value[:, N:]


def rows_times(value, wide):
    parts = jnp.concatenate(split_value(value), axis=1)
    return halves_added(jnp.dot(parts, wide, preferred_element_type=jnp.float32))


def times_block(row, value):
    parts = jnp.concatenate(split_value(value), axis=1)
    parts = jnp.concatenate([parts, parts], axis=0)
    return halves_added(jnp.dot(row, parts, preferred_element_type=jnp.float32))


def shifted_groups(items, group):
    for bit in (1, 2, 4):
        moved = group // bit % 2 == 1
        items = [jnp.where(moved, items[(at + bit) % 8], items[at]) for at in range(8)]
    return items


def turned_groups(items):
    group = lax.broadcasted_iota(jnp.int32, items[0].shape, 1) // 16
    items = shifted_groups(items, group)
    items = items[:1] + [pltpu.roll(items[at], at * 16, 1) for at in range(1, 8)]
    items = shifted_groups(items, group)
    return [items[-at % 8] for at in range(8)]


def node_sum(rel, fields, node):
    out = jnp.zeros_like(fields[0])
    for offset in range(4):
        out = jnp.where(rel == node - (offset - 1), fields[offset], out)
    return out


def frequency(positions):
    return jnp.where(positions < N // 2, positions, positions - N)


def phi_kernel(table_ref, near_ref, out_ref, flat_ref, shell_ref, fraction_ref, stage_ref, group_ref, sems):
    flat_ref[...] = jnp.zeros_like(flat_ref)
    start = 0
    for node in range(NA):
        count = NA - node
        flat_ref[start : start + count, 0 : table_ref.shape[2]] = table_ref[node, node:NA, :]
        start += count
    table = split_value(flat_ref[...])
    band_at, grid_at = lax.axis_index("band"), lax.axis_index("grid")
    wave_set = band_at * 2 + grid_at // 8
    point = lax.broadcasted_iota(jnp.int32, (PHI_POINTS, N), 0)
    slot = point // 16
    other = jnp.where(wave_set == 0, 32, 64 - wave_set)
    freq_y = frequency(jnp.where(slot < 2, wave_set, other) + slot % 2 * 64)
    freq_z = frequency(point % 16 + grid_at % 8 * 16)
    freq_x = frequency(lax.broadcasted_iota(jnp.int32, (PHI_POINTS, N), 1))
    square = freq_x * freq_x + freq_z * freq_z + freq_y * freq_y
    root = jnp.sqrt(square.astype(jnp.float32))
    shell = root.astype(jnp.int32)
    shell = shell - (shell * shell > square).astype(jnp.int32)
    shell = shell + ((shell + 1) * (shell + 1) <= square).astype(jnp.int32)
    shell_ref[...] = shell
    fraction_ref[...] = root - shell.astype(jnp.float32)
    row = lax.broadcasted_iota(jnp.int32, (N, N), 0)

    def weights(at):
        low = shell_ref[pl.ds(at, 1), :]
        part = fraction_ref[pl.ds(at, 1), :]
        return jnp.where(row == low, 1.0 - part, jnp.where(row == low + 1, part, 0.0))

    def put(step):
        slot = step % 2
        return pltpu.make_async_copy(group_ref.at[slot], out_ref.at[step], sems.at[slot])

    def group(step, carry):
        for pair in range(4):
            first = step * 8 + pair * 2
            both = jnp.concatenate([weights(first), weights(first + 1)], axis=1)
            value = product(table, split_value(both))
            stage_ref[pair * 2 * PAIR_ROWS : (pair * 2 + 1) * PAIR_ROWS, :] = value[:, :N]
            stage_ref[(pair * 2 + 1) * PAIR_ROWS : (pair * 2 + 2) * PAIR_ROWS, :] = value[:, N:]

        @pl.when(step >= 2)
        def _():
            put(step - 2).wait()

        for item in range(PAIRS):
            group_ref[step % 2, item] = stage_ref[pl.ds(item, 8, stride=PAIR_ROWS), :]
        put(step).start()

        @pl.when(step < 2)
        def _():
            near_ref[step] = group_ref[step % 2]

        return carry

    lax.fori_loop(0, GROUPS, group, 0)
    put(GROUPS - 2).wait()
    put(GROUPS - 1).wait()


def fields_kernel(
    index_ref, weight_ref, slope_ref, theta_out, slope_out,
    index_buf, weight_buf, slope_buf, sems,
):
    band_at = lax.axis_index("band")
    plane = band_at // 2
    copies = [
        pltpu.make_async_copy(index_ref.at[plane], index_buf, sems.at[0]),
        pltpu.make_async_copy(weight_ref.at[:, plane], weight_buf, sems.at[1]),
        pltpu.make_async_copy(slope_ref.at[:, plane], slope_buf, sems.at[2]),
    ]
    for copy in copies:
        copy.start()
    for copy in copies:
        copy.wait()
    rows = pl.ds(band_at % 2, 64, stride=2)
    rel = index_buf[rows, :]
    for buf, out_ref in ((weight_buf, theta_out), (slope_buf, slope_out)):
        fields = [buf[offset, rows, :] for offset in range(4)]
        for node in range(NA):
            out_ref[node] = node_sum(rel, fields, node)


def sort_kernel(far_ref, out_ref, plane_ref, sorted_ref, in_sems, out_sems):
    def get(plane):
        return pltpu.make_async_copy(far_ref.at[plane], plane_ref.at[plane], in_sems.at[plane])

    def put(plane):
        return pltpu.make_async_copy(
            sorted_ref.at[pl.ds(2 * plane, 2)], out_ref.at[pl.ds(2 * plane, 2)], out_sems.at[plane]
        )

    for plane in range(8):
        get(plane).start()
    for plane in range(8):
        get(plane).wait()
        for parity in range(2):
            sorted_ref[2 * plane + parity] = plane_ref[plane, pl.ds(parity, 64, stride=2), :]
        put(plane).start()
    for plane in range(8):
        put(plane).wait()


def forward_kernel(parts_ref, coefficient_ref, cas_ref, half_ref, far_ref, out_ref, near_ref, sems):
    paired = lax.axis_index("band") * 2 + lax.axis_index("grid") // 8 != 0
    copies = [
        pltpu.make_async_copy(far_ref.at[2 + step], near_ref.at[step], sems.at[step])
        for step in range(2)
    ]

    @pl.when(jnp.logical_not(paired))
    def _():
        for copy in copies:
            copy.start()

    density = parts_ref[0]
    for part in range(1, 16):
        density = density + parts_ref[part]
    row = half_ref[...]
    theta = density[None] * coefficient_ref[...]
    along_z = rows_times(theta.reshape(NA * 64, N), cas_ref[...])
    for pair in range(ROWS):
        items = []
        for node in range(4 * pair, 4 * pair + 4):
            waves = times_block(row, along_z[node * 64 : (node + 1) * 64])
            items += [waves[:32], waves[32:]]
        for block, item in enumerate(turned_groups(items)):
            out_ref[pl.ds(block * ROWS + pair, 32, stride=8 * ROWS), :] = item

    @pl.when(jnp.logical_not(paired))
    def _():
        for copy in copies:
            copy.wait()


def mix_kernel(
    data_ref, cas_ref, twist_ref, first_ref, second_ref, far_ref, out_ref,
    spec_ref, mixed_ref, late_ref, sems,
):
    cas = cas_ref[...]
    wave_set = lax.axis_index("band") * 2 + lax.axis_index("grid") // 8
    paired = wave_set != 0
    last = jnp.where(paired, 2, 4)
    late = [
        pltpu.make_async_copy(far_ref.at[last + step], late_ref.at[step], sems.at[step])
        for step in range(2)
    ]
    for copy in late:
        copy.start()

    twist = [twist_ref[pl.ds(wave_set * 4 + factor, 1), :] for factor in range(4)]

    def lines(half, pair, at):
        return pl.ds((at * 2 + half) * 16 * ROWS + pair, 16, stride=ROWS)

    for pair in range(ROWS):
        even, odd = (
            rows_times(
                jnp.concatenate([data_ref[lines(half, pair, at), :] for at in range(8)], axis=0).T,
                cas,
            )
            for half in range(2)
        )
        for at in range(4):
            start = (4 * pair + at) * POINTS
            near, other = odd[at * 32 : at * 32 + 16], odd[at * 32 + 16 : at * 32 + 32]
            turned = (
                twist[0] * near + twist[1] * other,
                twist[2] * near + twist[3] * other,
            )
            for residue in range(2):
                first = even[at * 32 + 16 * residue : at * 32 + 16 * residue + 16]
                base = start + 32 * residue
                spec_ref[base : base + 16, :] = first + turned[residue]
                spec_ref[base + 16 : base + 32, :] = first - turned[residue]

    def group(step, phi_at):
        spec = [spec_ref[pl.ds(node * POINTS + step * 8, 8), :] for node in range(NA)]
        total = [None] * NA
        item = 0
        for a in range(NA):
            for b in range(a, NA):
                phi = phi_at[item]
                item += 1
                term = phi * spec[a]
                total[b] = term if total[b] is None else total[b] + term
                if a != b:
                    term = phi * spec[b]
                    total[a] = term if total[a] is None else total[a] + term
        for b in range(NA):
            mixed_ref[pl.ds(b * POINTS + step * 8, 8), :] = total[b]

    def each(start, count, gap, phi_of):
        def body(turn, carry):
            group(start + gap * turn, phi_of(turn))
            return carry

        lax.fori_loop(0, count, body, 0)

    each(0, 2, 1, lambda turn: first_ref.at[turn])

    @pl.when(paired)
    def _():
        each(6, 2, 1, lambda turn: first_ref.at[turn])

    @pl.when(jnp.logical_not(paired))
    def _():
        each(2, 2, 1, lambda turn: second_ref.at[turn])

    for step in range(2):
        late[step].wait()
        each(last + step, 2, 2, lambda turn, step=step: late_ref.at[step])

    for pair in range(ROWS):
        even, odd = [], []
        for node in range(4 * pair, 4 * pair + 4):
            start = node * POINTS
            slots = [mixed_ref[start + 16 * slot : start + 16 * slot + 16, :] for slot in range(4)]
            even += [slots[0] + slots[1], slots[2] + slots[3]]
            near, other = slots[0] - slots[1], slots[2] - slots[3]
            odd += [twist[0] * near + twist[1] * other, twist[2] * near + twist[3] * other]
        for half, rows in enumerate((even, odd)):
            block = times_block(cas[:N], jnp.concatenate(rows, axis=0).T)
            for at in range(8):
                out_ref[lines(half, pair, at), :] = block[at * 16 : at * 16 + 16]


def inverse_kernel(data_ref, coefficient_ref, cas_ref, half_ref, out_ref):
    cas, row = cas_ref[...], half_ref[...]
    along_y = []
    for pair in range(ROWS):
        items = turned_groups(
            [data_ref[pl.ds(block * ROWS + pair, 32, stride=8 * ROWS), :] for block in range(8)]
        )
        for at in range(4):
            waves = jnp.concatenate([items[2 * at], items[2 * at + 1]], axis=0)
            along_y.append(times_block(row, waves))
    fields = rows_times(jnp.concatenate(along_y, axis=0), cas)
    total = fields[:64] * coefficient_ref[0]
    for node in range(1, NA):
        total = total + fields[node * 64 : (node + 1) * 64] * coefficient_ref[node]
    out_ref[...] = total * (1.0 / float(N) ** 3)


def weave_kernel(data_ref, out_ref, plane_ref, sems):
    copies = []
    for plane in range(8):
        for parity in range(2):
            plane_ref[plane, pl.ds(parity, 64, stride=2), :] = data_ref[2 * plane + parity]
        copies.append(
            pltpu.make_async_copy(plane_ref.at[plane], out_ref.at[plane], sems.at[plane])
        )
        copies[-1].start()
    for copy in copies:
        copy.wait()


def vmem():
    return pl.BlockSpec(memory_space=pltpu.VMEM)


def anywhere():
    return pl.BlockSpec(memory_space=pl.ANY)


def far(value):
    return pltpu.with_memory_space_constraint(value, pltpu.HBM)


def per_device(partial_density, node_index, node_weight, node_slope, kernel_table):
    table = cas_table()
    cas = split_constant(table)
    half = half_table()
    x_order = np.arange(N).reshape(16, 8).T.reshape(-1)
    cas_x = split_constant(table[x_order])
    axes = ("band", "grid")
    f32 = jnp.float32

    phi_first, phi_far = pl.pallas_call(
        phi_kernel,
        out_shape=[
            pltpu.VMEM((2, PAIRS, 8, N), f32),
            pltpu.HBM((GROUPS, PAIRS, 8, N), f32),
        ],
        in_specs=[vmem()],
        out_specs=[vmem(), anywhere()],
        scratch_shapes=[
            pltpu.VMEM((PAIR_ROWS, N), f32),
            pltpu.VMEM((PHI_POINTS, N), jnp.int32),
            pltpu.VMEM((PHI_POINTS, N), f32),
            pltpu.VMEM((8 * PAIR_ROWS, N), f32),
            pltpu.VMEM((2, PAIRS, 8, N), f32),
            pltpu.SemaphoreType.DMA((2,)),
        ],
        compiler_params=pltpu.CompilerParams(vmem_limit_bytes=8 << 20),
        cost_estimate=pl.CostEstimate(flops=4 * 10**9, bytes_accessed=8 << 20, transcendentals=0),
        name="phi",
    )(kernel_table)

    theta, slope = pl.pallas_call(
        fields_kernel,
        out_shape=[pltpu.VMEM((NA, 64, N), f32), pltpu.HBM((NA, 64, N), f32)],
        in_specs=[anywhere()] * 3,
        out_specs=[vmem()] * 2,
        scratch_shapes=[
            pltpu.VMEM((N, N), jnp.int32),
            pltpu.VMEM((4, N, N), f32),
            pltpu.VMEM((4, N, N), f32),
            pltpu.SemaphoreType.DMA((3,)),
        ],
        compiler_params=pltpu.CompilerParams(vmem_limit_bytes=4 << 20),
        cost_estimate=pl.CostEstimate(flops=10**8, bytes_accessed=2 << 20, transcendentals=0),
        name="fields",
    )(far(node_index), far(node_weight), far(node_slope))
    rows = pl.pallas_call(
        sort_kernel,
        out_shape=pltpu.HBM((16, 64, N), f32),
        in_specs=[anywhere()],
        out_specs=anywhere(),
        scratch_shapes=[
            pltpu.VMEM((8, N, N), f32),
            pltpu.VMEM((16, 64, N), f32),
            pltpu.SemaphoreType.DMA((8,)),
            pltpu.SemaphoreType.DMA((8,)),
        ],
        compiler_params=pltpu.CompilerParams(vmem_limit_bytes=4 << 20),
        name="sort_rows",
    )(far(partial_density[0]))
    parts = lax.all_to_all(rows, "band", 0, 0, tiled=True)
    parts, phi_first, phi_far, slope, theta = lax.optimization_barrier(
        (parts, phi_first, phi_far, slope, theta)
    )
    lines, phi_second = pl.pallas_call(
        forward_kernel,
        out_shape=[
            jax.ShapeDtypeStruct((256 * ROWS, N), f32),
            pltpu.VMEM((2, PAIRS, 8, N), f32),
        ],
        in_specs=[vmem()] * 4 + [anywhere()],
        out_specs=[vmem()] * 2,
        scratch_shapes=[pltpu.SemaphoreType.DMA((2,))],
        compiler_params=pltpu.CompilerParams(vmem_limit_bytes=12 << 20),
        name="forward",
    )(parts, theta, cas, split_row(half.T), far(phi_far))
    lines = lax.all_to_all(lines.reshape(256, 1, ROWS * N), axes, 0, 0, tiled=True)
    lines = lines.reshape(256 * ROWS, N)
    lines = pl.pallas_call(
        mix_kernel,
        out_shape=jax.ShapeDtypeStruct((256 * ROWS, N), f32),
        in_specs=[vmem()] * 5 + [anywhere()],
        out_specs=vmem(),
        scratch_shapes=[
            pltpu.VMEM((NA * POINTS, N), f32),
            pltpu.VMEM((NA * POINTS, N), f32),
            pltpu.VMEM((2, PAIRS, 8, N), f32),
            pltpu.SemaphoreType.DMA((2,)),
        ],
        compiler_params=pltpu.CompilerParams(vmem_limit_bytes=24 << 20),
        name="mix",
    )(lines, cas_x, twist_table(), phi_first, phi_second, far(phi_far))
    lines = lax.all_to_all(lines.reshape(256, 1, ROWS * N), axes, 0, 0, tiled=True)
    lines = lines.reshape(256 * ROWS, N)
    share = pl.pallas_call(
        inverse_kernel,
        out_shape=jax.ShapeDtypeStruct((64, N), f32),
        in_specs=[vmem()] * 4,
        out_specs=vmem(),
        compiler_params=pltpu.CompilerParams(vmem_limit_bytes=12 << 20),
        name="inverse",
    )(lines, slope, cas, split_row(half))
    gathered = lax.all_to_all(
        jnp.broadcast_to(share[None], (16, 64, N)), "band", 0, 0, tiled=True
    )
    return pl.pallas_call(
        weave_kernel,
        out_shape=pltpu.HBM((8, N, N), f32),
        in_specs=[vmem()],
        out_specs=anywhere(),
        scratch_shapes=[pltpu.VMEM((8, N, N), f32), pltpu.SemaphoreType.DMA((8,))],
        compiler_params=pltpu.CompilerParams(vmem_limit_bytes=4 << 20),
        name="weave",
    )(gathered)


def solution(mesh):
    placed = (
        P("band", "grid", None, None),
        P("grid", None, None),
        P(None, "grid", None, None),
        P(None, "grid", None, None),
        P(),
    )
    return jax.shard_map(
        per_device, mesh=mesh, in_specs=placed, out_specs=P("grid", None, None), check_vma=False
    )
```
